256 devices in a mesh: dp: 32 (over z, y), mp: 8 (over x, core).
Axes of the slice: x: 4, y: 4, z: 8, core: 2. Of those that a mesh axis runs over, the one named last changes fastest.
Arguments:
- features: bfloat16 [3, 512, 65536], P(None, 'mp', 'dp'), may hold values from -6 to 6
- weights: bfloat16 [11, 512, 512], P(None, 'mp'), may hold values from -0.25 to 0.25
- sample_owner: int32 [3, 65536, 1], P(None, 'dp'), may hold values from 0 to 31; in each aligned block of 2048 rows (0 to 2047, 2048 to 4095, ..., all dimensions but the last counted through in order) at most 128 rows name the same one
- sample_row: int32 [3, 65536], P(None, 'dp'), may hold values from 0 to 2047
- edge_src: int32 [8, 65536], P(None, 'dp'), may hold values from 0 to 2047
- edge_dst: int32 [8, 65536], P(None, 'dp'), may hold values from 0 to 127
- edge_count: int32 [8, 32], P(None, 'dp'), may hold values from 128 to 2048
Outputs:
- updated: bfloat16 [3, 512, 4096], P(None, 'mp', 'dp')
The draws below stay inside these ranges and needn't reach their ends.
Inputs may be any that keep to these rules, and one draw needn't show every extreme that they name: `sample_owner`: among the 2048 entries of one node type in one block no owner appears more than 128 times; some owner appears exactly 128 times in some blocks.
All inputs are finite; a program needn't handle non-finite values.
Results may differ from the reference program's by a relative error of at most 0.0064.
Values may be sent and summed in bfloat16 or wider, within the bound.
A program may use at most 64 MiB of HBM per device.

```python
import math
import jax
import jax.numpy as jnp
import numpy as np
from jax import lax

D = 512
RELS = 8
TYPES = 3
MATS = 11
ROWS_DEV = 2048
SAMP = 2048
SEEDS = 128
EDGES = 2048
CAP = 128
TABLE_ROWS = 65536
SAMPLES = 65536
EDGES_ALL = 65536
N_DP = 32


def plant(values, stream_key, smallest, high):
    extent = values.shape
    spot = [jax.random.randint(jax.random.fold_in(stream_key, axis), (), 0, extent[axis]) for axis in range(len(extent))]
    values = values.at[tuple(spot)].set(smallest)
    longest = extent.index(max(extent))
    spot[longest] = (spot[longest] + 1) % extent[longest]
    return values.at[tuple(spot)].set(high)


def level_of(rng, shape, cuts, low, largest):
    loudness = 1.0
    for position, shards_of in cuts:
        draws = jax.random.uniform(jax.random.fold_in(jax.random.fold_in(rng, 6), position), (shards_of,), jnp.float32, low / len(cuts), largest / len(cuts))
        loudness = loudness * jnp.repeat(jnp.exp(draws), shape[position] // shards_of).reshape((-1,) + (1,) * (len(shape) - 1 - position))
    return loudness


def assign_block(own_key, own, number, rows, count, top, limit, lean):
    sequence = jax.random.permutation(own_key, count)
    heavy_load, common = portions_of(count, rows * top, limit, lean, True), portions_of(count, rows * top, limit, lean, False)
    places = jnp.arange(count)

    def named(tallies, rotation):
        used = int((tallies > 0).sum())
        fixed = max(1, used // 4)
        passed = fixed + (places - fixed + rotation * (used - fixed)) % max(1, count - fixed)
        return jnp.zeros((count,), jnp.int32).at[sequence[jnp.where(places < fixed, places, passed)]].set(jnp.asarray(tallies, jnp.int32))

    tallies = jnp.where(number % 4 == 0, named(heavy_load, number // 4), named(common, number - number // 4 - 1))
    mixed = jax.random.permutation(jax.random.fold_in(own, 3), count)
    source_of, sink = mixed[0:count // 2 * 2:2], mixed[1:count // 2 * 2:2]
    margin = jnp.minimum(tallies[source_of] - 1, limit - tallies[sink]) // 2
    margin = jnp.where((source_of == sequence[0]) | (sink == sequence[0]) | (tallies[sink] == 0), 0, jnp.maximum(margin, 0))
    passed = jax.random.randint(jax.random.fold_in(own, 4), (count // 2,), 0, 1 << 20) % (margin + 1)
    tallies = tallies.at[source_of].add(-passed).at[sink].add(passed)
    labels = jnp.searchsorted(jnp.cumsum(tallies), jnp.arange(rows * top), side="right").astype(jnp.int32)
    listing = labels.reshape(top, rows).T
    listing = listing[jax.random.permutation(jax.random.fold_in(own, 1), rows)]
    rotation = jax.random.randint(jax.random.fold_in(own, 2), (rows, 1), 0, top)
    return jnp.take_along_axis(listing, (jnp.arange(top)[None, :] + rotation) % top, axis=1)


def portions_of(count, total, limit, skew, full):
    loads = [(1 << 20) // math.isqrt(standing ** skew) + 1 for standing in range(1, count + 1)]
    largest = limit if full else min(limit, max(-(-total // count), total * loads[0] // sum(loads)))
    least = 1 if total - largest >= count - 1 else 0
    given, rest = [largest] + [least] * (count - 1), total - largest - least * (count - 1)
    while rest > 0:
        free = [i for i in range(1, count) if given[i] < largest] or [i for i in range(1, count) if given[i] < limit]
        whole, left = sum([loads[i] for i in free]), rest
        for i in free:
            more = min(limit - given[i], max(1, left * loads[i] // whole), rest)
            given[i] = given[i] + more
            rest = rest - more
    return np.array(given)


def normal_values(key, dims, width, most, split=(), kind=jnp.bfloat16):
    drawn = jax.random.normal(key, dims, jnp.float32) * width
    if len(split) > 0:
        drawn = level_of(key, dims, split, -0.22, 0.18) * drawn
    return jnp.clip(drawn, min=-most, max=most).astype(kind)


def setup_inputs(seed: int = 0) -> dict:
    arg_keys = jax.random.split(jax.random.key(seed), 8)
    features = normal_values(arg_keys[0], (TYPES, D, TABLE_ROWS), 1.0, 6.0, ((1, 8), (2, 32)))
    weights = normal_values(arg_keys[1], (MATS, D, D), D ** -0.5, 0.25, ((1, 8),))
    sample_owner_keys = jax.random.split(jax.random.fold_in(arg_keys[2], 1), TYPES * SAMPLES // SAMP)
    sample_owner_turns = jax.random.permutation(jax.random.fold_in(arg_keys[2], 3), TYPES * SAMPLES // SAMP)
    sample_owner = jax.vmap(lambda own, number: assign_block(jax.random.fold_in(arg_keys[2], 2), own, number, SAMP, N_DP, 1, CAP, 2))(sample_owner_keys, sample_owner_turns).reshape((TYPES, SAMPLES, 1))
    sample_row = plant(jax.random.randint(arg_keys[3], (TYPES, SAMPLES), 0, ROWS_DEV), jax.random.fold_in(arg_keys[3], 1), 0, ROWS_DEV - 1).astype(jnp.int32)
    edge_src = plant(jax.random.randint(arg_keys[4], (RELS, EDGES_ALL), 0, SAMP), jax.random.fold_in(arg_keys[4], 1), 0, SAMP - 1).astype(jnp.int32)
    edge_dst = plant(jax.random.randint(arg_keys[5], (RELS, EDGES_ALL), 0, SEEDS), jax.random.fold_in(arg_keys[5], 1), 0, SEEDS - 1).astype(jnp.int32)
    edge_count = plant(jax.random.randint(arg_keys[6], (RELS, N_DP), EDGES // 16, EDGES + 1), jax.random.fold_in(arg_keys[6], 1), EDGES // 16, EDGES).astype(jnp.int32)
    return {"features": features, "weights": weights, "sample_owner": sample_owner, "sample_row": sample_row, "edge_src": edge_src, "edge_dst": edge_dst, "edge_count": edge_count}


RELATION_SOURCE = (0, 1, 0, 1, 2, 0, 2, 1)
RELATION_TARGET = (1, 0, 0, 2, 1, 2, 0, 1)


def reference(features, weights, sample_owner, sample_row, edge_src, edge_dst, edge_count):
    row_index = (sample_owner[:, :, 0] * ROWS_DEV + sample_row).astype(jnp.int32)
    block_index = row_index.reshape(TYPES, N_DP, SAMP).transpose(1, 0, 2)
    block_src = edge_src.reshape(RELS, N_DP, EDGES).transpose(1, 0, 2)
    block_dst = edge_dst.reshape(RELS, N_DP, EDGES).transpose(1, 0, 2)
    block_count = edge_count.transpose(1, 0)

    def one_block(inputs):
        index_here, src_here, dst_here, count_here = inputs
        fetched = [jnp.take(features[node_kind], index_here[node_kind], axis=1).T for node_kind in range(TYPES)]
        typed = [jnp.dot(fetched[node_kind][:SEEDS], weights[RELS + node_kind], preferred_element_type=jnp.float32) for node_kind in range(TYPES)]
        slot_ids = jnp.arange(EDGES, dtype=jnp.int32)
        for relation in range(RELS):
            live_edge = (slot_ids < count_here[relation]).astype(jnp.float32)
            sources = jnp.take(fetched[RELATION_SOURCE[relation]], src_here[relation], axis=0).astype(jnp.float32)
            summed = jax.ops.segment_sum(sources * live_edge[:, None], dst_here[relation], num_segments=SEEDS)
            degree = jax.ops.segment_sum(live_edge, dst_here[relation], num_segments=SEEDS)
            message = (summed / jnp.maximum(degree, 1.0)[:, None]).astype(jnp.bfloat16)
            target = RELATION_TARGET[relation]
            typed[target] = typed[target] + jnp.dot(message, weights[relation], preferred_element_type=jnp.float32)
        return jnp.stack([jax.nn.relu(value).astype(jnp.bfloat16) for value in typed])

    result = lax.map(one_block, (block_index, block_src, block_dst, block_count))
    return result.transpose(1, 3, 0, 2).reshape(TYPES, result.shape[3], N_DP * SEEDS)
```

```python
import functools

import jax
import jax.numpy as jnp
from jax import lax
from jax.experimental import pallas as pl
from jax.experimental.pallas import tpu as pltpu
from jax.sharding import PartitionSpec as P

TYPES = 3
RELS = 8
SEEDS = 128
CAP = 128
RELATION_SOURCE = (0, 1, 0, 1, 2, 0, 2, 1)
STACKS = ((1, 2, 6, 8), (0, 4, 7, 9), (3, 5, 10))
NZ, NY = 8, 4
DP = NZ * NY
MESH = pl.DeviceIdType.MESH
F32, BF16, I32 = jnp.float32, jnp.bfloat16, jnp.int32
EB = 512


def iota(shape, dim):
    return lax.broadcasted_iota(I32, shape, dim)


def hot(ids, rows):
    return (iota((rows, ids.shape[1]), 0) == ids).astype(F32).astype(BF16)


def dot(a, b):
    return jnp.dot(a, b, preferred_element_type=F32)


def dot_nt(a, b):
    return lax.dot_general(a, b, (((1,), (1,)), ((), ())), preferred_element_type=F32)


def kernel(n_mp, feat, w, own, row, esrc, edst, ecnt, out, rq, req_out, req_in, send, recv,
           lk, pc, plo, msgs, wt, psend, precv, rs, rr, ss, sr, ps, pr):
    me, mm = lax.axis_index("dp"), lax.axis_index("mp")
    z, y = me // NY, me % NY

    def fwd(s):
        return ((z + s // NY) % NZ) * NY + (y + s % NY) % NY

    def bwd(s):
        return ((z + NZ - s // NY) % NZ) * NY + (y + NY - s % NY) % NY

    barrier = pltpu.get_barrier_semaphore()

    def greet(s, _):
        pl.semaphore_signal(barrier, 1, device_id={"dp": fwd(s)}, device_id_type=MESH)
        return 0

    lax.fori_loop(1, DP, greet, 0)

    def greet_mp(d, _):
        pl.semaphore_signal(barrier, 1, device_id={"mp": (mm + d) % n_mp}, device_id_type=MESH)
        return 0

    lax.fori_loop(1, n_mp, greet_mp, 0)

    upper = (iota((256, 256), 0) <= iota((256, 256), 1)).astype(F32).astype(BF16)
    base = jnp.zeros((TYPES * DP, 1), F32)
    acc = [jnp.zeros((2 * DP, CAP), F32) for _ in range(TYPES)]
    for blk in range(8):
        lanes = slice(blk * 256, (blk + 1) * 256)
        owners = [own[t, :, lanes] for t in range(TYPES)]
        ohs = [(iota((DP, 256), 0) == owners[t]).astype(F32) for t in range(TYPES)]
        oh = jnp.concatenate(ohs, axis=0)
        incl = dot(oh.astype(BF16), upper) + base
        base = incl[:, 255:256]
        ranked = oh * (incl - 1.0)
        for t in range(TYPES):
            rank = jnp.sum(ranked[t * DP:(t + 1) * DP], axis=0, keepdims=True).astype(I32)
            ids = row[t:t + 1, lanes]
            left = jnp.concatenate(
                [ohs[t] * (ids >> 8).astype(F32), ohs[t] * (ids & 255).astype(F32)], axis=0
            ).astype(BF16)
            acc[t] = acc[t] + dot_nt(left, hot(rank, CAP))
            lk[t, blk:blk + 1, :] = (owners[t] >> 1).astype(F32)
            lk[t, 8 + blk:9 + blk, :] = ((owners[t] & 1) * CAP + rank).astype(F32)
    for t in range(TYPES):
        rq[t * DP:(t + 1) * DP, :] = (acc[t][:DP] * 256.0 + acc[t][DP:]).astype(I32)
    for o in range(DP):
        req_out[o, :, :] = rq[pl.ds(o, TYPES, stride=DP), :]

    pl.semaphore_wait(barrier, DP - 1 + n_mp - 1)

    def req_copy(s):
        return pltpu.make_async_remote_copy(
            req_out.at[fwd(s)], req_in.at[me], rs.at[s], rr.at[s],
            device_id={"dp": fwd(s)}, device_id_type=MESH)

    def ask(s, _):
        req_copy(s).start()
        return 0

    lax.fori_loop(1, DP, ask, 0)
    req_in[me] = req_out[me]

    def row_copy(t, s):
        return pltpu.make_async_remote_copy(
            send.at[t, bwd(s)], recv.at[t, me], ss.at[t, s], sr.at[t, s],
            device_id={"dp": bwd(s)}, device_id_type=MESH)

    def serve(t, dz, first):
        peers = [bwd(dz * NY + j) for j in range(NY)]
        if t == 0:
            for j in range(NY):
                if not (first and j == 0):
                    req_copy(dz * NY + j).wait_recv()
        ids = jnp.concatenate([req_in[peers[j], t:t + 1, :] for j in range(NY)], axis=1)
        low, high = ids & 255, ids >> 8
        table = jnp.concatenate([feat[t, :, c * 256:(c + 1) * 256] for c in range(8)], axis=0)
        res = dot(table, hot(low, 256))
        picked = res[0:64]
        for c in range(1, 8):
            picked = jnp.where(high == c, res[c * 64:(c + 1) * 64], picked)
        picked = picked.astype(BF16)
        for j in range(NY):
            piece = picked[:, j * CAP:(j + 1) * CAP]
            if first and j == 0:
                recv[t, me] = piece
            else:
                send[t, peers[j]] = piece
        for j in range(NY):
            if not (first and j == 0):
                row_copy(t, dz * NY + j).start()

    def zorder(i):
        return (i % 2) * ((i + 1) // 2) + (1 - i % 2) * ((NZ - i // 2) % NZ)

    for t in range(TYPES):
        serve(t, 0, True)

        def step(i, _, t=t):
            serve(t, zorder(i), False)
            return 0

        lax.fori_loop(1, NZ, step, 0)

    for r in range(RELS):
        t = RELATION_SOURCE[r]

        def look(k, _, r=r, t=t):
            lanes = pl.ds(pl.multiple_of(k * EB, EB), EB)
            src = esrc[r:r + 1, lanes]
            res = dot(lk[t].astype(BF16), hot(src & 255, 256))
            here = iota((8, EB), 0) == (src >> 8)
            pc[r:r + 1, lanes] = jnp.sum(jnp.where(here, res[:8], 0.0), axis=0, keepdims=True)
            plo[r:r + 1, lanes] = jnp.sum(jnp.where(here, res[8:], 0.0), axis=0, keepdims=True)
            return 0

        lax.fori_loop(0, 2048 // EB, look, 0)

    for a in range(TYPES):
        mats = [w[m].astype(F32) for m in STACKS[a]]
        if len(mats) < 4:
            mats.append(jnp.zeros_like(mats[0]))
            msgs[a, 192:256, :] = jnp.zeros((64, SEEDS), BF16)
        wt[a] = jnp.concatenate(mats, axis=0).T.astype(BF16)

    def pick(t, chunk, low):
        oh = hot(low.astype(I32), 256)
        picked = None
        for g in range(4):
            left = jnp.concatenate(
                [jnp.concatenate([recv[t, 2 * c], recv[t, 2 * c + 1]], axis=1)
                 for c in range(4 * g, 4 * g + 4)], axis=0)
            res = dot(left, oh)
            for k in range(4):
                part = res[k * 64:(k + 1) * 64]
                picked = part if picked is None else jnp.where(chunk == float(4 * g + k), part, picked)
        return picked.astype(BF16)

    def place(m):
        for a in range(TYPES):
            if m in STACKS[a]:
                return a, STACKS[a].index(m) * 64

    for t in range(TYPES):
        def land(s, _, t=t):
            row_copy(t, s).wait_recv()
            return 0

        lax.fori_loop(1, DP, land, 0)
        a, k = place(RELS + t)
        msgs[a, k:k + 64, :] = pick(t, lk[t, 0:1, 0:SEEDS], lk[t, 8:9, 0:SEEDS])
        for r in range(RELS):
            if RELATION_SOURCE[r] != t:
                continue
            count = ecnt[0, r]

            def edges(k, total, r=r, t=t, count=count):
                lanes = pl.ds(pl.multiple_of(k * EB, EB), EB)
                rows = pick(t, pc[r:r + 1, lanes], plo[r:r + 1, lanes])
                rows = jnp.concatenate([rows, jnp.ones((16, EB), BF16)], axis=0)
                slot = iota((1, EB), 1) + k * EB
                target = jnp.where(slot < count, edst[r:r + 1, lanes], -1)
                return total + dot_nt(rows, hot(target, SEEDS))

            total = lax.fori_loop(0, 2048 // EB, edges, jnp.zeros((80, SEEDS), F32))
            a, k = place(r)
            msgs[a, k:k + 64, :] = (total[:64] / jnp.maximum(total[64:65], 1.0)).astype(BF16)

    def part_copy(a, d):
        return pltpu.make_async_remote_copy(
            psend.at[a, (mm + d) % n_mp], precv.at[a, mm], ps.at[a, d], pr.at[a, d],
            device_id={"mp": (mm + d) % n_mp}, device_id_type=MESH)

    for a in range(TYPES):
        part = dot(wt[a], msgs[a]).astype(BF16)
        for p in range(n_mp):
            psend[a, p] = part[p * 64:(p + 1) * 64]
        for d in range(1, n_mp):
            part_copy(a, d).start()
        precv[a, mm] = psend[a, mm]
    for a in range(TYPES):
        for d in range(1, n_mp):
            part_copy(a, d).wait_recv()
        typed = precv[a, 0].astype(F32)
        for p in range(1, n_mp):
            typed = typed + precv[a, p].astype(F32)
        out[a] = jnp.maximum(typed, 0.0).astype(BF16)

    def drain(s, _):
        req_copy(s).wait_send()
        for t in range(TYPES):
            row_copy(t, s).wait_send()
        return 0

    lax.fori_loop(1, DP, drain, 0)
    for a in range(TYPES):
        for d in range(1, n_mp):
            part_copy(a, d).wait_send()


def solution(mesh):
    n_mp = mesh.shape["mp"]

    def per_device(features, weights, sample_owner, sample_row, edge_src, edge_dst, edge_count):
        vmem = pl.BlockSpec(memory_space=pltpu.VMEM)
        return pl.pallas_call(
            functools.partial(kernel, n_mp),
            out_shape=jax.ShapeDtypeStruct((TYPES, 64, SEEDS), BF16),
            in_specs=[vmem] * 6 + [pl.BlockSpec(memory_space=pltpu.SMEM)],
            out_specs=vmem,
            scratch_shapes=[
                pltpu.VMEM((TYPES * DP, CAP), I32),
                pltpu.VMEM((DP, TYPES, CAP), I32),
                pltpu.VMEM((DP, TYPES, CAP), I32),
                pltpu.VMEM((TYPES, DP, 64, CAP), BF16),
                pltpu.VMEM((TYPES, DP, 64, CAP), BF16),
                pltpu.VMEM((TYPES, 16, 256), F32),
                pltpu.VMEM((RELS, 2048), F32),
                pltpu.VMEM((RELS, 2048), F32),
                pltpu.VMEM((TYPES, 256, SEEDS), BF16),
                pltpu.VMEM((TYPES, 512, 256), BF16),
                pltpu.VMEM((TYPES, n_mp, 64, SEEDS), BF16),
                pltpu.VMEM((TYPES, n_mp, 64, SEEDS), BF16),
                pltpu.SemaphoreType.DMA((DP,)),
                pltpu.SemaphoreType.DMA((DP,)),
                pltpu.SemaphoreType.DMA((TYPES, DP)),
                pltpu.SemaphoreType.DMA((TYPES, DP)),
                pltpu.SemaphoreType.DMA((TYPES, n_mp)),
                pltpu.SemaphoreType.DMA((TYPES, n_mp)),
            ],
            compiler_params=pltpu.CompilerParams(
                collective_id=0, has_side_effects=True, vmem_limit_bytes=56 << 20),
        )(features, weights, jnp.transpose(sample_owner, (0, 2, 1)), sample_row,
          edge_src, edge_dst, jnp.transpose(edge_count, (1, 0)))

    return jax.shard_map(
        per_device,
        mesh=mesh,
        in_specs=(
            P(None, "mp", "dp"),
            P(None, "mp", None),
            P(None, "dp", None),
            P(None, "dp"),
            P(None, "dp"),
            P(None, "dp"),
            P(None, "dp"),
        ),
        out_specs=P(None, "mp", "dp"),
        check_vma=False,
    )
```

```python
import jax
import jax.numpy as jnp
from jax import lax
from jax.experimental import pallas as pl
from jax.experimental.pallas import tpu as pltpu
from jax.sharding import PartitionSpec as P

TYPES = 3
RELS = 8
SEEDS = 128
CAP = 128
RELATION_SOURCE = (0, 1, 0, 1, 2, 0, 2, 1)
STACKS = ((1, 2, 6, 8), (0, 4, 7, 9), (3, 5, 10))
NZ, NY = 8, 4
DP = NZ * NY
MESH = pl.DeviceIdType.MESH
F32, BF16, I32 = jnp.float32, jnp.bfloat16, jnp.int32
EB = 512


def iota(shape, dim):
    return lax.broadcasted_iota(I32, shape, dim)


def hot(ids, rows):
    return (iota((rows, ids.shape[1]), 0) == ids).astype(F32).astype(BF16)


def dot(a, b):
    return jnp.dot(a, b, preferred_element_type=F32)


def dot_nt(a, b):
    return lax.dot_general(a, b, (((1,), (1,)), ((), ())), preferred_element_type=F32)


def hops(o):
    return min(o[0], NZ - o[0]) + min(o[1], NY - o[1])


OFFSETS = [(dz, dy) for dz in range(NZ) for dy in range(NY)]
NEAREST = sorted(OFFSETS, key=lambda o: (hops(o), o[1], o[0]))
PLANES = (4, 3, 5, 2, 6, 1, 7, 0)
LAST = 2
LAST_RELS = tuple(r for r in range(RELS) if RELATION_SOURCE[r] == LAST)


def kernel(feat_h, w_h, own_h, row_h, esrc_h, edst_h, ecnt_h, out,
           feat, w, own, row, esrc, edst, ecnt,
           rq, req_out, req_in, send, recv, lk, pc, plo, lohot, counts, deg, msgs, wt,
           psend, pair, comb, final, ins, rs, rr, ss, sr, ds, dr, ps, pr):
    me, mm = lax.axis_index("dp"), lax.axis_index("mp")
    z, y = me // NY, me % NY
    x, core = mm // 2, mm % 2
    nx = final.shape[1]

    def fwd(o):
        return ((z + o[0]) % NZ) * NY + (y + o[1]) % NY

    def bwd(o):
        return ((z + NZ - o[0]) % NZ) * NY + (y + NY - o[1]) % NY

    def sem(o):
        return o[0] * NY + o[1]

    barrier = pltpu.get_barrier_semaphore()
    for o in NEAREST[:0:-1]:
        pl.semaphore_signal(barrier, 1, device_id={"dp": fwd(o)}, device_id_type=MESH)
    sibling = x * 2 + (1 - core)
    pl.semaphore_signal(barrier, 1, device_id={"mp": sibling}, device_id_type=MESH)

    def along_x(d):
        return ((x + d) % nx) * 2 + core

    for d in range(1, nx):
        pl.semaphore_signal(barrier, 1, device_id={"mp": along_x(d)}, device_id_type=MESH)

    loads = [
        pltpu.make_async_copy(src, dst, ins.at[i])
        for i, (src, dst) in enumerate((
            (own_h, own), (row_h, row), (feat_h, feat), (esrc_h, esrc), (edst_h, edst),
            (ecnt_h, ecnt), (w_h, w)))
    ]
    for load in loads:
        load.start()

    upper = (iota((256, 256), 0) <= iota((256, 256), 1)).astype(F32).astype(BF16)
    base = jnp.zeros((TYPES * DP, 1), F32)
    acc = [jnp.zeros((2 * DP, CAP), F32) for _ in range(TYPES)]
    loads[0].wait()
    loads[1].wait()
    for blk in range(8):
        lanes = slice(blk * 256, (blk + 1) * 256)
        owners = [own[t, :, lanes] for t in range(TYPES)]
        ohs = [(iota((DP, 256), 0) == owners[t]).astype(F32) for t in range(TYPES)]
        oh = jnp.concatenate(ohs, axis=0)
        incl = dot(oh.astype(BF16), upper) + base
        base = incl[:, 255:256]
        ranked = oh * (incl - 1.0)
        for t in range(TYPES):
            rank = jnp.sum(ranked[t * DP:(t + 1) * DP], axis=0, keepdims=True).astype(I32)
            ids = row[t:t + 1, lanes]
            left = jnp.concatenate(
                [ohs[t] * (ids >> 8).astype(F32), ohs[t] * (ids & 255).astype(F32)], axis=0
            ).astype(BF16)
            acc[t] = acc[t] + dot_nt(left, hot(rank, CAP))
            lk[t, blk:blk + 1, :] = (owners[t] >> 1).astype(F32)
            lk[t, 8 + blk:9 + blk, :] = ((owners[t] & 1) * CAP + rank).astype(F32)
    for t in range(TYPES):
        rq[t * DP:(t + 1) * DP, :] = (acc[t][:DP] * 256.0 + acc[t][DP:]).astype(I32)
    for o in range(DP):
        req_out[o, :, :] = rq[pl.ds(o, TYPES, stride=DP), :]

    pl.semaphore_wait(barrier, DP - 1 + nx)

    def req_copy(o):
        return pltpu.make_async_remote_copy(
            req_out.at[fwd(o)], req_in.at[me], rs.at[sem(o)], rr.at[sem(o)],
            device_id={"dp": fwd(o)}, device_id_type=MESH)

    for o in NEAREST[:0:-1]:
        req_copy(o).start()
    req_in[me] = req_out[me]

    def row_copy(t, o):
        return pltpu.make_async_remote_copy(
            send.at[t, bwd(o)], recv.at[t, me], ss.at[t, sem(o)], sr.at[t, sem(o)],
            device_id={"dp": bwd(o)}, device_id_type=MESH)

    asked = {(0, 0)}

    def serve(t, group):
        for o in group:
            if o not in asked:
                req_copy(o).wait_recv()
                asked.add(o)
        peers = [bwd(o) for o in group]
        ids = jnp.concatenate([req_in[p, t:t + 1, :] for p in peers], axis=1)
        low, high = ids & 255, ids >> 8
        table = jnp.concatenate([feat[t, :, c * 256:(c + 1) * 256] for c in range(8)], axis=0)
        res = dot(table, hot(low, 256))
        picked = res[0:64]
        for c in range(1, 8):
            picked = jnp.where(high == c, res[c * 64:(c + 1) * 64], picked)
        picked = picked.astype(BF16)
        for j, o in enumerate(group):
            piece = picked[:, j * CAP:(j + 1) * CAP]
            if o == (0, 0):
                recv[t, me] = piece
            else:
                send[t, peers[j]] = piece
        for o in group:
            if o != (0, 0):
                row_copy(t, o).start()

    groups = [NEAREST[4 * g:4 * g + 4] for g in range(8)]
    loads[2].wait()
    for t, gs in ((0, groups[:4]), (1, groups[:4]), (0, groups[4:]), (1, groups[4:])):
        for g in gs:
            serve(t, g)
    for dz in PLANES:
        serve(LAST, [(dz, dy) for dy in range(NY)])

    loads[3].wait()
    for r in range(RELS):
        t = RELATION_SOURCE[r]

        def look(k, _, r=r, t=t):
            lanes = pl.ds(pl.multiple_of(k * EB, EB), EB)
            src = esrc[r:r + 1, lanes]
            res = dot(lk[t].astype(BF16), hot(src & 255, 256))
            here = iota((8, EB), 0) == (src >> 8)
            pc[r:r + 1, lanes] = jnp.sum(jnp.where(here, res[:8], 0.0), axis=0, keepdims=True)
            plo[r:r + 1, lanes] = jnp.sum(jnp.where(here, res[8:], 0.0), axis=0, keepdims=True)
            return 0

        lax.fori_loop(0, 2048 // EB, look, 0)
    loads[4].wait()
    loads[5].wait()
    loads[6].wait()

    for i, r in enumerate(LAST_RELS):
        slot = iota((1, 2048), 1)
        target = jnp.where(slot < ecnt[0, r], edst[r:r + 1, :], -1)
        deg[i] = dot_nt(jnp.ones((16, 2048), BF16), hot(target, SEEDS))
        lohot[...] = hot(plo[r:r + 1, :].astype(I32), 256)

        def count(n, _, i=i, r=r):
            slot = iota((1, 2048), 1)
            pair_id = jnp.where(slot < ecnt[0, r],
                                pc[r:r + 1, :].astype(I32) * SEEDS + edst[r:r + 1, :] - n * 256, -1)
            res = dot_nt(lohot[...], hot(pair_id, 256)).astype(BF16)
            counts[2 * n, :, i * SEEDS:(i + 1) * SEEDS] = res[:, :SEEDS]
            counts[2 * n + 1, :, i * SEEDS:(i + 1) * SEEDS] = res[:, SEEDS:]
            return 0

        lax.fori_loop(0, 8, count, 0)
    for c in range(16):
        seed = jnp.where(lk[LAST, 0:1, 0:SEEDS] == float(c), lk[LAST, 8:9, 0:SEEDS], -1.0)
        counts[c, :, 256:384] = hot(seed.astype(I32), 256)

    for a in range(TYPES):
        mats = [w[m].astype(F32) for m in STACKS[a]]
        if len(mats) < 4:
            mats.append(jnp.zeros_like(mats[0]))
            msgs[a, 192:256, :] = jnp.zeros((64, SEEDS), BF16)
        wt[a] = jnp.concatenate(mats, axis=0).T.astype(BF16)

    def landed(t, c):
        return jnp.concatenate([recv[t, 2 * c], recv[t, 2 * c + 1]], axis=1)

    def pick(t, chunk, low):
        oh = hot(low.astype(I32), 256)
        picked = None
        for g in range(4):
            left = jnp.concatenate([landed(t, c) for c in range(4 * g, 4 * g + 4)], axis=0)
            res = dot(left, oh)
            for k in range(4):
                part = res[k * 64:(k + 1) * 64]
                picked = part if picked is None else jnp.where(chunk == float(4 * g + k), part, picked)
        return picked.astype(BF16)

    def put(m, value):
        for a in range(TYPES):
            if m in STACKS[a]:
                k = STACKS[a].index(m) * 64
                msgs[a, k:k + 64, :] = value.astype(BF16)

    for t in range(LAST):
        for o in NEAREST[1:]:
            row_copy(t, o).wait_recv()
        put(RELS + t, pick(t, lk[t, 0:1, 0:SEEDS], lk[t, 8:9, 0:SEEDS]))
        for r in range(RELS):
            if RELATION_SOURCE[r] != t:
                continue
            live = ecnt[0, r]

            def edges(k, total, r=r, t=t, live=live):
                lanes = pl.ds(pl.multiple_of(k * EB, EB), EB)
                rows = pick(t, pc[r:r + 1, lanes], plo[r:r + 1, lanes])
                rows = jnp.concatenate([rows, jnp.ones((16, EB), BF16)], axis=0)
                slot = iota((1, EB), 1) + k * EB
                target = jnp.where(slot < live, edst[r:r + 1, lanes], -1)
                return total + dot_nt(rows, hot(target, SEEDS))

            total = lax.fori_loop(0, 2048 // EB, edges, jnp.zeros((80, SEEDS), F32))
            put(r, total[:64] / jnp.maximum(total[64:65], 1.0))

    total = jnp.zeros((64, 384), F32)
    for dz in PLANES:
        for dy in range(NY):
            if (dz, dy) != (0, 0):
                row_copy(LAST, (dz, dy)).wait_recv()
        for h in range(2):
            c = ((z + dz) % NZ) * 2 + h
            total = total + dot(landed(LAST, c), counts[c])
    for i, r in enumerate(LAST_RELS):
        put(r, total[:, i * SEEDS:(i + 1) * SEEDS] / jnp.maximum(deg[i, 0:1, :], 1.0))
    put(RELS + LAST, total[:, 256:384])

    def pair_copy(a):
        return pltpu.make_async_remote_copy(
            psend.at[a, 1 - core], pair.at[a], ds.at[a], dr.at[a],
            device_id={"mp": sibling}, device_id_type=MESH)

    def part_copy(a, d):
        return pltpu.make_async_remote_copy(
            comb.at[a, (x + d) % nx], final.at[a, x], ps.at[a, d], pr.at[a, d],
            device_id={"mp": along_x(d)}, device_id_type=MESH)

    for a in range(TYPES):
        part = dot(wt[a], msgs[a]).astype(BF16)
        for p in range(2 * nx):
            psend[a, p % 2, p // 2] = part[p * 64:(p + 1) * 64]
        pair_copy(a).start()
    for a in range(TYPES):
        pair_copy(a).wait_recv()
        comb[a] = (psend[a, core].astype(F32) + pair[a].astype(F32)).astype(BF16)
        for d in range(1, nx):
            part_copy(a, d).start()
        final[a, x] = comb[a, x]
    for a in range(TYPES):
        for d in range(1, nx):
            part_copy(a, d).wait_recv()
        typed = final[a, 0].astype(F32)
        for p in range(1, nx):
            typed = typed + final[a, p].astype(F32)
        out[a] = jnp.maximum(typed, 0.0).astype(BF16)

    for o in NEAREST[1:]:
        req_copy(o).wait_send()
        for t in range(TYPES):
            row_copy(t, o).wait_send()
    for a in range(TYPES):
        pair_copy(a).wait_send()
        for d in range(1, nx):
            part_copy(a, d).wait_send()


def solution(mesh):
    n_mp = mesh.shape["mp"]

    def per_device(features, weights, sample_owner, sample_row, edge_src, edge_dst, edge_count):
        nx = n_mp // 2
        return pl.pallas_call(
            kernel,
            out_shape=jax.ShapeDtypeStruct((TYPES, 64, SEEDS), BF16),
            in_specs=[pl.BlockSpec(memory_space=pltpu.HBM)] * 7,
            out_specs=pl.BlockSpec(memory_space=pltpu.VMEM),
            scratch_shapes=[
                pltpu.VMEM((TYPES, 64, 2048), BF16),
                pltpu.VMEM((11, 64, 512), BF16),
                pltpu.VMEM((TYPES, 1, 2048), I32),
                pltpu.VMEM((TYPES, 2048), I32),
                pltpu.VMEM((RELS, 2048), I32),
                pltpu.VMEM((RELS, 2048), I32),
                pltpu.SMEM((1, RELS), I32),
                pltpu.VMEM((TYPES * DP, CAP), I32),
                pltpu.VMEM((DP, TYPES, CAP), I32),
                pltpu.VMEM((DP, TYPES, CAP), I32),
                pltpu.VMEM((TYPES, DP, 64, CAP), BF16),
                pltpu.VMEM((TYPES, DP, 64, CAP), BF16),
                pltpu.VMEM((TYPES, 16, 256), F32),
                pltpu.VMEM((RELS, 2048), F32),
                pltpu.VMEM((RELS, 2048), F32),
                pltpu.VMEM((256, 2048), BF16),
                pltpu.VMEM((16, 256, 384), BF16),
                pltpu.VMEM((len(LAST_RELS), 16, SEEDS), F32),
                pltpu.VMEM((TYPES, 256, SEEDS), BF16),
                pltpu.VMEM((TYPES, 512, 256), BF16),
                pltpu.VMEM((TYPES, 2, nx, 64, SEEDS), BF16),
                pltpu.VMEM((TYPES, nx, 64, SEEDS), BF16),
                pltpu.VMEM((TYPES, nx, 64, SEEDS), BF16),
                pltpu.VMEM((TYPES, nx, 64, SEEDS), BF16),
                pltpu.SemaphoreType.DMA((7,)),
                pltpu.SemaphoreType.DMA((DP,)),
                pltpu.SemaphoreType.DMA((DP,)),
                pltpu.SemaphoreType.DMA((TYPES, DP)),
                pltpu.SemaphoreType.DMA((TYPES, DP)),
                pltpu.SemaphoreType.DMA((TYPES,)),
                pltpu.SemaphoreType.DMA((TYPES,)),
                pltpu.SemaphoreType.DMA((TYPES, nx)),
                pltpu.SemaphoreType.DMA((TYPES, nx)),
            ],
            compiler_params=pltpu.CompilerParams(
                collective_id=0, has_side_effects=True, vmem_limit_bytes=60000000),
        )(features, weights, jnp.transpose(sample_owner, (0, 2, 1)), sample_row,
          edge_src, edge_dst, jnp.transpose(edge_count, (1, 0)))

    return jax.shard_map(
        per_device,
        mesh=mesh,
        in_specs=(
            P(None, "mp", "dp"),
            P(None, "mp", None),
            P(None, "dp", None),
            P(None, "dp"),
            P(None, "dp"),
            P(None, "dp"),
            P(None, "dp"),
        ),
        out_specs=P(None, "mp", "dp"),
        check_vma=False,
    )
```

```python
import jax
import jax.numpy as jnp
from jax import lax
from jax.experimental import pallas as pl
from jax.experimental.pallas import tpu as pltpu
from jax.sharding import PartitionSpec as P

TYPES = 3
RELS = 8
SEEDS = 128
CAP = 128
RELATION_SOURCE = (0, 1, 0, 1, 2, 0, 2, 1)
STACKS = ((1, 2, 6, 8), (0, 4, 7, 9), (3, 5, 10))
NZ, NY = 8, 4
DP = NZ * NY
MESH = pl.DeviceIdType.MESH
F32, BF16, I32 = jnp.float32, jnp.bfloat16, jnp.int32
EB = 512


def iota(shape, dim):
    return lax.broadcasted_iota(I32, shape, dim)


def hot(ids, rows):
    return (iota((rows, ids.shape[1]), 0) == ids).astype(F32).astype(BF16)


def dot(a, b):
    return jnp.dot(a, b, preferred_element_type=F32)


def dot_nt(a, b):
    return lax.dot_general(a, b, (((1,), (1,)), ((), ())), preferred_element_type=F32)


def hops(o):
    return min(o[0], NZ - o[0]) + min(o[1], NY - o[1])


OFFSETS = [(dz, dy) for dz in range(NZ) for dy in range(NY)]
NEAREST = sorted(OFFSETS, key=lambda o: (hops(o), o[1], o[0]))
PLANES = (4, 3, 5, 2, 6, 1, 7, 0)
LAST = 2
PARTS = 2
PART = 64 // PARTS
PIECES = 8 + 3 * PARTS
FARTHEST = (4, 3, 5, 2, 6, 1, 7)
LAST_RELS = tuple(r for r in range(RELS) if RELATION_SOURCE[r] == LAST)


def kernel(feat_h, w_h, own_h, row_h, esrc_h, edst_h, ecnt_h, out,
           feat, w, own, row, esrc, edst, ecnt,
           rq, req_out, req_in, send, recv, lk, pc, plo, lohot, counts, deg, msgs, wt,
           wfull, mfull, ins, rs, rr, ss, sr, ls, lr, ws, wr, ms, mr):
    me, mm = lax.axis_index("dp"), lax.axis_index("mp")
    z, y = me // NY, me % NY
    n_mp = mfull.shape[1]

    def fwd(o):
        return ((z + o[0]) % NZ) * NY + (y + o[1]) % NY

    def bwd(o):
        return ((z + NZ - o[0]) % NZ) * NY + (y + NY - o[1]) % NY

    def sem(o):
        return o[0] * NY + o[1]

    barrier = pltpu.get_barrier_semaphore()
    for o in NEAREST[:0:-1]:
        pl.semaphore_signal(barrier, 1, device_id={"dp": fwd(o)}, device_id_type=MESH)
    for d in range(1, n_mp):
        pl.semaphore_signal(barrier, 1, device_id={"mp": (mm + d) % n_mp}, device_id_type=MESH)

    loads = [
        pltpu.make_async_copy(src, dst, ins.at[i])
        for i, (src, dst) in enumerate((
            (own_h, own), (row_h, row), (feat_h, feat), (esrc_h, esrc), (edst_h, edst),
            (ecnt_h, ecnt), (w_h, w)))
    ]
    for load in loads:
        load.start()

    upper = (iota((256, 256), 0) <= iota((256, 256), 1)).astype(F32).astype(BF16)
    base = jnp.zeros((TYPES * DP, 1), F32)
    acc = [jnp.zeros((2 * DP, CAP), F32) for _ in range(TYPES)]
    loads[0].wait()
    loads[1].wait()
    for blk in range(8):
        lanes = slice(blk * 256, (blk + 1) * 256)
        owners = [own[t, :, lanes] for t in range(TYPES)]
        ohs = [(iota((DP, 256), 0) == owners[t]).astype(F32) for t in range(TYPES)]
        oh = jnp.concatenate(ohs, axis=0)
        incl = dot(oh.astype(BF16), upper) + base
        base = incl[:, 255:256]
        ranked = oh * (incl - 1.0)
        for t in range(TYPES):
            rank = jnp.sum(ranked[t * DP:(t + 1) * DP], axis=0, keepdims=True).astype(I32)
            ids = row[t:t + 1, lanes]
            left = jnp.concatenate(
                [ohs[t] * (ids >> 8).astype(F32), ohs[t] * (ids & 255).astype(F32)], axis=0
            ).astype(BF16)
            acc[t] = acc[t] + dot_nt(left, hot(rank, CAP))
            lk[t, blk:blk + 1, :] = (owners[t] >> 1).astype(F32)
            lk[t, 8 + blk:9 + blk, :] = ((owners[t] & 1) * CAP + rank).astype(F32)
    for t in range(TYPES):
        rq[t * DP:(t + 1) * DP, :] = (acc[t][:DP] * 256.0 + acc[t][DP:]).astype(I32)
    for o in range(DP):
        req_out[o, :, :] = rq[pl.ds(o, TYPES, stride=DP), :]

    pl.semaphore_wait(barrier, DP - 1 + n_mp - 1)

    def req_copy(o):
        return pltpu.make_async_remote_copy(
            req_out.at[fwd(o)], req_in.at[me], rs.at[sem(o)], rr.at[sem(o)],
            device_id={"dp": fwd(o)}, device_id_type=MESH)

    for o in NEAREST[:0:-1]:
        req_copy(o).start()
    req_in[me] = req_out[me]

    def row_copy(t, o):
        return pltpu.make_async_remote_copy(
            send.at[t, bwd(o)], recv.at[t, me], ss.at[t, sem(o)], sr.at[t, sem(o)],
            device_id={"dp": bwd(o)}, device_id_type=MESH)

    def last_copy(h, o):
        rows = pl.ds(h * PART, PART)
        return pltpu.make_async_remote_copy(
            send.at[LAST, bwd(o), rows, :], recv.at[LAST, me, rows, :],
            ls.at[h, sem(o)], lr.at[h, sem(o)],
            device_id={"dp": bwd(o)}, device_id_type=MESH)

    asked = {(0, 0)}

    def serve(t, group):
        for o in group:
            if o not in asked:
                req_copy(o).wait_recv()
                asked.add(o)
        peers = [bwd(o) for o in group]
        ids = jnp.concatenate([req_in[p, t:t + 1, :] for p in peers], axis=1)
        low, high = ids & 255, ids >> 8
        table = jnp.concatenate([feat[t, :, c * 256:(c + 1) * 256] for c in range(8)], axis=0)
        res = dot(table, hot(low, 256))
        picked = res[0:64]
        for c in range(1, 8):
            picked = jnp.where(high == c, res[c * 64:(c + 1) * 64], picked)
        picked = picked.astype(BF16)
        for j, o in enumerate(group):
            piece = picked[:, j * CAP:(j + 1) * CAP]
            if o == (0, 0):
                recv[t, me] = piece
            else:
                send[t, peers[j]] = piece
        for o in group:
            if o != (0, 0):
                (last_copy(0, o) if t == LAST else row_copy(t, o)).start()

    groups = [NEAREST[4 * g:4 * g + 4] for g in range(8)]
    loads[2].wait()
    for t, gs in ((0, groups[:4]), (1, groups[:4]), (0, groups[4:]), (1, groups[4:])):
        for g in gs:
            serve(t, g)
    for dz in PLANES:
        serve(LAST, [(dz, dy) for dy in range(NY)])
    for h in range(1, PARTS):
        for dz in PLANES:
            for dy in range(NY):
                if (dz, dy) != (0, 0):
                    last_copy(h, (dz, dy)).start()

    def w_copy(a, d):
        p = (mm + d) % n_mp
        return pltpu.make_async_remote_copy(
            wt.at[a, pl.ds(pl.multiple_of(p * 64, 64), 64), :], wfull.at[a, mm],
            ws.at[a, d], wr.at[a, d], device_id={"mp": p}, device_id_type=MESH)

    loads[6].wait()
    for a in range(TYPES):
        mats = [w[m].astype(F32) for m in STACKS[a]]
        if len(mats) < 4:
            mats.append(jnp.zeros_like(mats[0]))
            for p in range(n_mp):
                mfull[a, p, 192:256, :] = jnp.zeros((64, SEEDS), BF16)
        wt[a] = jnp.concatenate(mats, axis=0).T.astype(BF16)
        for d in FARTHEST:
            w_copy(a, d).start()
        wfull[a, mm] = wt[a, pl.ds(pl.multiple_of(mm * 64, 64), 64), :]

    loads[3].wait()
    for r in range(RELS):
        t = RELATION_SOURCE[r]

        def look(k, _, r=r, t=t):
            lanes = pl.ds(pl.multiple_of(k * EB, EB), EB)
            src = esrc[r:r + 1, lanes]
            res = dot(lk[t].astype(BF16), hot(src & 255, 256))
            here = iota((8, EB), 0) == (src >> 8)
            pc[r:r + 1, lanes] = jnp.sum(jnp.where(here, res[:8], 0.0), axis=0, keepdims=True)
            plo[r:r + 1, lanes] = jnp.sum(jnp.where(here, res[8:], 0.0), axis=0, keepdims=True)
            return 0

        lax.fori_loop(0, 2048 // EB, look, 0)
    loads[4].wait()
    loads[5].wait()

    for i, r in enumerate(LAST_RELS):
        slot = iota((1, 2048), 1)
        target = jnp.where(slot < ecnt[0, r], edst[r:r + 1, :], -1)
        deg[i] = dot_nt(jnp.ones((16, 2048), BF16), hot(target, SEEDS))
        lohot[...] = hot(plo[r:r + 1, :].astype(I32), 256)

        def count(n, _, i=i, r=r):
            slot = iota((1, 2048), 1)
            pair_id = jnp.where(slot < ecnt[0, r],
                                pc[r:r + 1, :].astype(I32) * SEEDS + edst[r:r + 1, :] - n * 256, -1)
            res = dot_nt(lohot[...], hot(pair_id, 256)).astype(BF16)
            counts[2 * n, :, i * SEEDS:(i + 1) * SEEDS] = res[:, :SEEDS]
            counts[2 * n + 1, :, i * SEEDS:(i + 1) * SEEDS] = res[:, SEEDS:]
            return 0

        lax.fori_loop(0, 8, count, 0)
    for c in range(16):
        seed = jnp.where(lk[LAST, 0:1, 0:SEEDS] == float(c), lk[LAST, 8:9, 0:SEEDS], -1.0)
        counts[c, :, 256:384] = hot(seed.astype(I32), 256)

    def landed(t, c):
        return jnp.concatenate([recv[t, 2 * c], recv[t, 2 * c + 1]], axis=1)

    def pick(t, chunk, low):
        oh = hot(low.astype(I32), 256)
        picked = None
        for g in range(4):
            left = jnp.concatenate([landed(t, c) for c in range(4 * g, 4 * g + 4)], axis=0)
            res = dot(left, oh)
            for k in range(4):
                part = res[k * 64:(k + 1) * 64]
                picked = part if picked is None else jnp.where(chunk == float(4 * g + k), part, picked)
        return picked.astype(BF16)

    pieces = []

    def m_copy(i, d):
        a, k, n = pieces[i]
        p = (mm + d) % n_mp
        return pltpu.make_async_remote_copy(
            msgs.at[a, pl.ds(k, n), :], mfull.at[a, mm, pl.ds(k, n), :],
            ms.at[i, d], mr.at[i, d], device_id={"mp": p}, device_id_type=MESH)

    def put(m, value, part=0):
        for a in range(TYPES):
            if m in STACKS[a]:
                n = value.shape[0]
                k = STACKS[a].index(m) * 64 + part * n
                value = value.astype(BF16)
                msgs[a, k:k + n, :] = value
                mfull[a, mm, k:k + n, :] = value
                pieces.append((a, k, n))
                for d in FARTHEST:
                    m_copy(len(pieces) - 1, d).start()

    for t in range(LAST):
        for o in NEAREST[1:]:
            row_copy(t, o).wait_recv()
        put(RELS + t, pick(t, lk[t, 0:1, 0:SEEDS], lk[t, 8:9, 0:SEEDS]))
        for r in range(RELS):
            if RELATION_SOURCE[r] != t:
                continue
            live = ecnt[0, r]

            def edges(k, total, r=r, t=t, live=live):
                lanes = pl.ds(pl.multiple_of(k * EB, EB), EB)
                rows = pick(t, pc[r:r + 1, lanes], plo[r:r + 1, lanes])
                rows = jnp.concatenate([rows, jnp.ones((16, EB), BF16)], axis=0)
                slot = iota((1, EB), 1) + k * EB
                target = jnp.where(slot < live, edst[r:r + 1, lanes], -1)
                return total + dot_nt(rows, hot(target, SEEDS))

            total = lax.fori_loop(0, 2048 // EB, edges, jnp.zeros((80, SEEDS), F32))
            put(r, total[:64] / jnp.maximum(total[64:65], 1.0))

    for h in range(PARTS):
        total = jnp.zeros((PART, 384), F32)
        for dz in PLANES:
            for dy in range(NY):
                if (dz, dy) != (0, 0):
                    last_copy(h, (dz, dy)).wait_recv()
            for half in range(2):
                c = ((z + dz) % NZ) * 2 + half
                rows = slice(h * PART, (h + 1) * PART)
                left = jnp.concatenate(
                    [recv[LAST, 2 * c, rows, :], recv[LAST, 2 * c + 1, rows, :]], axis=1)
                total = total + dot(left, counts[c])
        for i, r in enumerate(LAST_RELS):
            put(r, total[:, i * SEEDS:(i + 1) * SEEDS] / jnp.maximum(deg[i, 0:1, :], 1.0), h)
        put(RELS + LAST, total[:, 256:384], h)

    for d in FARTHEST[::-1]:
        for a in range(TYPES):
            w_copy(a, d).wait_recv()
        for i in range(len(pieces)):
            m_copy(i, d).wait_recv()
    for a in range(TYPES):
        typed = dot(wfull[a, 0], mfull[a, 0])
        for p in range(1, n_mp):
            typed = typed + dot(wfull[a, p], mfull[a, p])
        out[a] = jnp.maximum(typed, 0.0).astype(BF16)

    for o in NEAREST[1:]:
        req_copy(o).wait_send()
        for t in range(LAST):
            row_copy(t, o).wait_send()
        for h in range(PARTS):
            last_copy(h, o).wait_send()
    for d in FARTHEST:
        for a in range(TYPES):
            w_copy(a, d).wait_send()
        for i in range(len(pieces)):
            m_copy(i, d).wait_send()


def solution(mesh):
    n_mp = mesh.shape["mp"]

    def per_device(features, weights, sample_owner, sample_row, edge_src, edge_dst, edge_count):
        return pl.pallas_call(
            kernel,
            out_shape=pltpu.VMEM((TYPES, 64, SEEDS), BF16),
            in_specs=[pl.BlockSpec(memory_space=pltpu.HBM)] * 7,
            out_specs=pl.BlockSpec(memory_space=pltpu.VMEM),
            scratch_shapes=[
                pltpu.VMEM((TYPES, 64, 2048), BF16),
                pltpu.VMEM((11, 64, 512), BF16),
                pltpu.VMEM((TYPES, 1, 2048), I32),
                pltpu.VMEM((TYPES, 2048), I32),
                pltpu.VMEM((RELS, 2048), I32),
                pltpu.VMEM((RELS, 2048), I32),
                pltpu.SMEM((1, RELS), I32),
                pltpu.VMEM((TYPES * DP, CAP), I32),
                pltpu.VMEM((DP, TYPES, CAP), I32),
                pltpu.VMEM((DP, TYPES, CAP), I32),
                pltpu.VMEM((TYPES, DP, 64, CAP), BF16),
                pltpu.VMEM((TYPES, DP, 64, CAP), BF16),
                pltpu.VMEM((TYPES, 16, 256), F32),
                pltpu.VMEM((RELS, 2048), F32),
                pltpu.VMEM((RELS, 2048), F32),
                pltpu.VMEM((256, 2048), BF16),
                pltpu.VMEM((16, 256, 384), BF16),
                pltpu.VMEM((len(LAST_RELS), 16, SEEDS), F32),
                pltpu.VMEM((TYPES, 256, SEEDS), BF16),
                pltpu.VMEM((TYPES, 512, 256), BF16),
                pltpu.VMEM((TYPES, n_mp, 64, 256), BF16),
                pltpu.VMEM((TYPES, n_mp, 256, SEEDS), BF16),
                pltpu.SemaphoreType.DMA((7,)),
                pltpu.SemaphoreType.DMA((DP,)),
                pltpu.SemaphoreType.DMA((DP,)),
                pltpu.SemaphoreType.DMA((LAST, DP)),
                pltpu.SemaphoreType.DMA((LAST, DP)),
                pltpu.SemaphoreType.DMA((PARTS, DP)),
                pltpu.SemaphoreType.DMA((PARTS, DP)),
                pltpu.SemaphoreType.DMA((TYPES, n_mp)),
                pltpu.SemaphoreType.DMA((TYPES, n_mp)),
                pltpu.SemaphoreType.DMA((PIECES, n_mp)),
                pltpu.SemaphoreType.DMA((PIECES, n_mp)),
            ],
            compiler_params=pltpu.CompilerParams(
                collective_id=0, has_side_effects=True, vmem_limit_bytes=60000000),
        )(features, weights, jnp.transpose(sample_owner, (0, 2, 1)), sample_row,
          edge_src, edge_dst, jnp.transpose(edge_count, (1, 0)))

    return jax.shard_map(
        per_device,
        mesh=mesh,
        in_specs=(
            P(None, "mp", "dp"),
            P(None, "mp", None),
            P(None, "dp", None),
            P(None, "dp"),
            P(None, "dp"),
            P(None, "dp"),
            P(None, "dp"),
        ),
        out_specs=P(None, "mp", "dp"),
        check_vma=False,
    )
```

```python
import jax
import jax.numpy as jnp
from jax import lax
from jax.experimental import pallas as pl
from jax.experimental.pallas import tpu as pltpu
from jax.sharding import PartitionSpec as P

TYPES = 3
RELS = 8
SEEDS = 128
CAP = 128
RELATION_SOURCE = (0, 1, 0, 1, 2, 0, 2, 1)
STACKS = ((1, 2, 6, 8), (0, 4, 7, 9), (3, 5, 10))
NZ, NY = 8, 4
DP = NZ * NY
MESH = pl.DeviceIdType.MESH
F32, BF16, I32 = jnp.float32, jnp.bfloat16, jnp.int32
EB = 512


def iota(shape, dim):
    return lax.broadcasted_iota(I32, shape, dim)


def hot(ids, rows):
    return (iota((rows, ids.shape[1]), 0) == ids).astype(F32).astype(BF16)


def dot(a, b):
    return jnp.dot(a, b, preferred_element_type=F32)


def dot_nt(a, b):
    return lax.dot_general(a, b, (((1,), (1,)), ((), ())), preferred_element_type=F32)


def hops(o):
    return min(o[0], NZ - o[0]) + min(o[1], NY - o[1])


OFFSETS = [(dz, dy) for dz in range(NZ) for dy in range(NY)]
NEAREST = sorted(OFFSETS, key=lambda o: (hops(o), o[1], o[0]))
PLANES = (4, 3, 5, 2, 6, 1, 7, 0)
LAST = 2
LAST_RELS = tuple(r for r in range(RELS) if RELATION_SOURCE[r] == LAST)


def kernel(feat_h, w_h, own_h, row_h, esrc_h, edst_h, ecnt_h, out,
           feat, w, own, row, esrc, edst, ecnt,
           rq, req_out, req_in, send, recv, lk, pc, plo, lohot, counts, deg, msgs, wt,
           gath, psend, precv, ins, rs, rr, ss, sr, lr, ps, pr):
    me, mm = lax.axis_index("dp"), lax.axis_index("mp")
    z, y = me // NY, me % NY
    n_mp = precv.shape[1]

    def fwd(o):
        return ((z + o[0]) % NZ) * NY + (y + o[1]) % NY

    def bwd(o):
        return ((z + NZ - o[0]) % NZ) * NY + (y + NY - o[1]) % NY

    groups = [NEAREST[4 * g:4 * g + 4] for g in range(8)]
    batch = {o: g for g in range(8) for o in groups[g]}

    def many(src, dst, send_sem, recv_sem):
        return pltpu.make_async_remote_copy(
            src, dst, send_sem, recv_sem, device_id={"dp": fwd((0, 1))}, device_id_type=MESH)

    barrier = pltpu.get_barrier_semaphore()
    for o in NEAREST[:0:-1]:
        pl.semaphore_signal(barrier, 1, device_id={"dp": fwd(o)}, device_id_type=MESH)
    for d in range(1, n_mp):
        pl.semaphore_signal(barrier, 1, device_id={"mp": (mm + d) % n_mp}, device_id_type=MESH)

    loads = [
        pltpu.make_async_copy(src, dst, ins.at[i])
        for i, (src, dst) in enumerate((
            (own_h, own), (row_h, row), (feat_h, feat), (esrc_h, esrc), (edst_h, edst),
            (ecnt_h, ecnt), (w_h, w)))
    ]
    for load in loads:
        load.start()

    upper = (iota((256, 256), 0) <= iota((256, 256), 1)).astype(F32).astype(BF16)
    base = jnp.zeros((TYPES * DP, 1), F32)
    acc = [jnp.zeros((2 * DP, CAP), F32) for _ in range(TYPES)]
    loads[0].wait()
    loads[1].wait()
    for blk in range(8):
        lanes = slice(blk * 256, (blk + 1) * 256)
        owners = [own[t, :, lanes] for t in range(TYPES)]
        ohs = [(iota((DP, 256), 0) == owners[t]).astype(F32) for t in range(TYPES)]
        oh = jnp.concatenate(ohs, axis=0)
        incl = dot(oh.astype(BF16), upper) + base
        base = incl[:, 255:256]
        ranked = oh * (incl - 1.0)
        for t in range(TYPES):
            rank = jnp.sum(ranked[t * DP:(t + 1) * DP], axis=0, keepdims=True).astype(I32)
            ids = row[t:t + 1, lanes]
            left = jnp.concatenate(
                [ohs[t] * (ids >> 8).astype(F32), ohs[t] * (ids & 255).astype(F32)], axis=0
            ).astype(BF16)
            acc[t] = acc[t] + dot_nt(left, hot(rank, CAP))
            lk[t, blk:blk + 1, :] = (owners[t] >> 1).astype(F32)
            lk[t, 8 + blk:9 + blk, :] = ((owners[t] & 1) * CAP + rank).astype(F32)
    for t in range(TYPES):
        rq[t * DP:(t + 1) * DP, :] = (acc[t][:DP] * 256.0 + acc[t][DP:]).astype(I32)
    for o in range(DP):
        req_out[o, :, :] = rq[pl.ds(o, TYPES, stride=DP), :]

    pl.semaphore_wait(barrier, DP - 1 + n_mp - 1)

    def req_copy(o):
        return pltpu.make_async_remote_copy(
            req_out.at[fwd(o)], req_in.at[me], rs.at[0], rr.at[batch[o]],
            device_id={"dp": fwd(o)}, device_id_type=MESH)

    for o in NEAREST[:0:-1]:
        req_copy(o).start()
    req_in[me] = req_out[me]

    def row_copy(t, o):
        return pltpu.make_async_remote_copy(
            send.at[t, bwd(o)], recv.at[t, me], ss.at[t],
            lr.at[o[0]] if t == LAST else sr.at[t],
            device_id={"dp": bwd(o)}, device_id_type=MESH)

    asked = set()

    def serve(t, group):
        for g in sorted({batch[o] for o in group} - asked):
            n = 3 if g == 0 else 4
            many(req_out.at[0:n], req_in.at[0:n], rs.at[0], rr.at[g]).wait_recv()
            asked.add(g)
        peers = [bwd(o) for o in group]
        ids = jnp.concatenate([req_in[p, t:t + 1, :] for p in peers], axis=1)
        low, high = ids & 255, ids >> 8
        table = jnp.concatenate([feat[t, :, c * 256:(c + 1) * 256] for c in range(8)], axis=0)
        res = dot(table, hot(low, 256))
        picked = res[0:64]
        for c in range(1, 8):
            picked = jnp.where(high == c, res[c * 64:(c + 1) * 64], picked)
        picked = picked.astype(BF16)
        for j, o in enumerate(group):
            piece = picked[:, j * CAP:(j + 1) * CAP]
            if o == (0, 0):
                recv[t, me] = piece
            else:
                send[t, peers[j]] = piece
        for o in group:
            if o != (0, 0):
                row_copy(t, o).start()

    loads[2].wait()
    for t, gs in ((0, groups[:4]), (1, groups[:4]), (0, groups[4:]), (1, groups[4:])):
        for g in gs:
            serve(t, g)
    for dz in PLANES:
        serve(LAST, [(dz, dy) for dy in range(NY)])

    loads[3].wait()
    for r in LAST_RELS:
        t = LAST

        def look(k, _, r=r, t=t):
            lanes = pl.ds(pl.multiple_of(k * EB, EB), EB)
            src = esrc[r:r + 1, lanes]
            res = dot(lk[t].astype(BF16), hot(src & 255, 256))
            here = iota((8, EB), 0) == (src >> 8)
            pc[r:r + 1, lanes] = jnp.sum(jnp.where(here, res[:8], 0.0), axis=0, keepdims=True)
            plo[r:r + 1, lanes] = jnp.sum(jnp.where(here, res[8:], 0.0), axis=0, keepdims=True)
            return 0

        lax.fori_loop(0, 2048 // EB, look, 0)
    loads[4].wait()
    loads[5].wait()
    loads[6].wait()

    for i, r in enumerate(LAST_RELS):
        slot = iota((1, 2048), 1)
        target = jnp.where(slot < ecnt[0, r], edst[r:r + 1, :], -1)
        deg[i] = dot_nt(jnp.ones((16, 2048), BF16), hot(target, SEEDS))
        lohot[...] = hot(plo[r:r + 1, :].astype(I32), 256)

        def count(n, _, i=i, r=r):
            slot = iota((1, 2048), 1)
            pair_id = jnp.where(slot < ecnt[0, r],
                                pc[r:r + 1, :].astype(I32) * SEEDS + edst[r:r + 1, :] - n * 256, -1)
            res = dot_nt(lohot[...], hot(pair_id, 256)).astype(BF16)
            counts[2 * n, :, i * SEEDS:(i + 1) * SEEDS] = res[:, :SEEDS]
            counts[2 * n + 1, :, i * SEEDS:(i + 1) * SEEDS] = res[:, SEEDS:]
            return 0

        lax.fori_loop(0, 8, count, 0)
    for c in range(16):
        seed = jnp.where(lk[LAST, 0:1, 0:SEEDS] == float(c), lk[LAST, 8:9, 0:SEEDS], -1.0)
        counts[c, :, 256:384] = hot(seed.astype(I32), 256)

    for a in range(TYPES):
        mats = [w[m].astype(F32) for m in STACKS[a]]
        if len(mats) < 4:
            mats.append(jnp.zeros_like(mats[0]))
            msgs[a, 192:256, :] = jnp.zeros((64, SEEDS), BF16)
        wt[a] = jnp.concatenate(mats, axis=0).T.astype(BF16)

    def landed(t, c):
        return jnp.concatenate([recv[t, 2 * c], recv[t, 2 * c + 1]], axis=1)

    def select(oh, chunk, parts):
        picked = None
        for g in range(0, len(parts), 4):
            res = dot(jnp.concatenate([part() for part in parts[g:g + 4]], axis=0), oh)
            for k in range(4):
                part = res[k * 64:(k + 1) * 64]
                picked = part if picked is None else jnp.where(chunk == g + k, part, picked)
        return picked.astype(BF16)

    def put(m, value):
        for a in range(TYPES):
            if m in STACKS[a]:
                k = STACKS[a].index(m) * 64
                msgs[a, k:k + 64, :] = value.astype(BF16)

    def all_rows(t, sems):
        return many(send.at[t, 0:DP - 1], recv.at[t, 0:DP - 1], ss.at[t], sems)

    many(req_out.at[0:DP - 1], req_in.at[0:DP - 1], rs.at[0], rr.at[0]).wait_send()
    for t in range(LAST):
        all_rows(t, sr.at[t]).wait_recv()

        def gather(k, _, t=t):
            chunk, low = (
                jnp.concatenate([lk[t, pl.ds(b + 2 * k, 1), :], lk[t, pl.ds(b + 2 * k + 1, 1), :]],
                                axis=1).astype(I32) for b in (0, 8))
            gath[:, pl.ds(pl.multiple_of(k * EB, EB), EB)] = select(
                hot(low, 256), chunk, [lambda c=c: landed(t, c) for c in range(16)])
            return 0

        lax.fori_loop(0, 2048 // EB, gather, 0)
        put(RELS + t, gath[:, 0:SEEDS])
        for r in range(RELS):
            if RELATION_SOURCE[r] != t:
                continue
            live = ecnt[0, r]

            def edges(k, total, r=r, live=live):
                lanes = pl.ds(pl.multiple_of(k * EB, EB), EB)
                src = esrc[r:r + 1, lanes]
                rows = select(hot(src & 255, 256), src >> 8,
                              [lambda c=c: gath[:, c * 256:(c + 1) * 256] for c in range(8)])
                rows = jnp.concatenate([rows, jnp.ones((16, EB), BF16)], axis=0)
                slot = iota((1, EB), 1) + k * EB
                target = jnp.where(slot < live, edst[r:r + 1, lanes], -1)
                return total + dot_nt(rows, hot(target, SEEDS))

            total = lax.fori_loop(0, 2048 // EB, edges, jnp.zeros((80, SEEDS), F32))
            put(r, total[:64] / jnp.maximum(total[64:65], 1.0))
        all_rows(t, sr.at[t]).wait_send()

    total = jnp.zeros((64, 384), F32)
    for dz in PLANES:
        n = NY - 1 if dz == 0 else NY
        many(send.at[LAST, 0:n], recv.at[LAST, 0:n], ss.at[LAST], lr.at[dz]).wait_recv()
        for h in range(2):
            c = ((z + dz) % NZ) * 2 + h
            total = total + dot(landed(LAST, c), counts[c])
    for i, r in enumerate(LAST_RELS):
        put(r, total[:, i * SEEDS:(i + 1) * SEEDS] / jnp.maximum(deg[i, 0:1, :], 1.0))
    put(RELS + LAST, total[:, 256:384])

    def part_copy(a, d):
        p = (mm + d) % n_mp
        return pltpu.make_async_remote_copy(
            psend.at[a, p], precv.at[a, mm], ps.at[0], pr.at[a],
            device_id={"mp": p}, device_id_type=MESH)

    for a in range(TYPES):
        part = dot(wt[a], msgs[a]).astype(BF16)
        for p in range(n_mp):
            psend[a, p] = part[p * 64:(p + 1) * 64]
        for d in (4, 3, 5, 2, 6, 1, 7):
            part_copy(a, d).start()
        precv[a, mm] = psend[a, mm]
    all_rows(LAST, sr.at[0]).wait_send()
    for a in range(TYPES):
        many(psend.at[a, 0:n_mp - 1], precv.at[a, 0:n_mp - 1], ps.at[0], pr.at[a]).wait_recv()
        typed = precv[a, 0].astype(F32)
        for p in range(1, n_mp):
            typed = typed + precv[a, p].astype(F32)
        out[a] = jnp.maximum(typed, 0.0).astype(BF16)
    many(psend.at[:, 0:n_mp - 1], precv.at[:, 0:n_mp - 1], ps.at[0], pr.at[0]).wait_send()


def solution(mesh):
    n_mp = mesh.shape["mp"]

    def per_device(features, weights, sample_owner, sample_row, edge_src, edge_dst, edge_count):
        return pl.pallas_call(
            kernel,
            out_shape=pltpu.VMEM((TYPES, 64, SEEDS), BF16),
            in_specs=[pl.BlockSpec(memory_space=pltpu.HBM)] * 7,
            out_specs=pl.BlockSpec(memory_space=pltpu.VMEM),
            scratch_shapes=[
                pltpu.VMEM((TYPES, 64, 2048), BF16),
                pltpu.VMEM((11, 64, 512), BF16),
                pltpu.VMEM((TYPES, 1, 2048), I32),
                pltpu.VMEM((TYPES, 2048), I32),
                pltpu.VMEM((RELS, 2048), I32),
                pltpu.VMEM((RELS, 2048), I32),
                pltpu.SMEM((1, RELS), I32),
                pltpu.VMEM((TYPES * DP, CAP), I32),
                pltpu.VMEM((DP, TYPES, CAP), I32),
                pltpu.VMEM((DP, TYPES, CAP), I32),
                pltpu.VMEM((TYPES, DP, 64, CAP), BF16),
                pltpu.VMEM((TYPES, DP, 64, CAP), BF16),
                pltpu.VMEM((TYPES, 16, 256), F32),
                pltpu.VMEM((RELS, 2048), F32),
                pltpu.VMEM((RELS, 2048), F32),
                pltpu.VMEM((256, 2048), BF16),
                pltpu.VMEM((16, 256, 384), BF16),
                pltpu.VMEM((len(LAST_RELS), 16, SEEDS), F32),
                pltpu.VMEM((TYPES, 256, SEEDS), BF16),
                pltpu.VMEM((TYPES, 512, 256), BF16),
                pltpu.VMEM((64, 2048), BF16),
                pltpu.VMEM((TYPES, n_mp, 64, SEEDS), BF16),
                pltpu.VMEM((TYPES, n_mp, 64, SEEDS), BF16),
                pltpu.SemaphoreType.DMA((7,)),
                pltpu.SemaphoreType.DMA((1,)),
                pltpu.SemaphoreType.DMA((8,)),
                pltpu.SemaphoreType.DMA((TYPES,)),
                pltpu.SemaphoreType.DMA((LAST,)),
                pltpu.SemaphoreType.DMA((NZ,)),
                pltpu.SemaphoreType.DMA((1,)),
                pltpu.SemaphoreType.DMA((TYPES,)),
            ],
            compiler_params=pltpu.CompilerParams(
                collective_id=0, has_side_effects=True, vmem_limit_bytes=60000000),
        )(features, weights, jnp.transpose(sample_owner, (0, 2, 1)), sample_row,
          edge_src, edge_dst, jnp.transpose(edge_count, (1, 0)))

    return jax.shard_map(
        per_device,
        mesh=mesh,
        in_specs=(
            P(None, "mp", "dp"),
            P(None, "mp", None),
            P(None, "dp", None),
            P(None, "dp"),
            P(None, "dp"),
            P(None, "dp"),
            P(None, "dp"),
        ),
        out_specs=P(None, "mp", "dp"),
        check_vma=False,
    )
```

```python
import jax
import jax.numpy as jnp
from jax import lax
from jax.experimental import pallas as pl
from jax.experimental.pallas import tpu as pltpu
from jax.sharding import PartitionSpec as P

TYPES = 3
RELS = 8
SEEDS = 128
CAP = 128
RELATION_SOURCE = (0, 1, 0, 1, 2, 0, 2, 1)
STACKS = ((1, 2, 6, 8), (0, 4, 7, 9), (3, 5, 10))
NZ, NY = 8, 4
DP = NZ * NY
MESH = pl.DeviceIdType.MESH
F32, BF16, I32 = jnp.float32, jnp.bfloat16, jnp.int32
EB = 512


def iota(shape, dim):
    return lax.broadcasted_iota(I32, shape, dim)


def hot(ids, rows):
    return (iota((rows, ids.shape[1]), 0) == ids).astype(F32).astype(BF16)


def dot(a, b):
    return jnp.dot(a, b, preferred_element_type=F32)


def dot_nt(a, b):
    return lax.dot_general(a, b, (((1,), (1,)), ((), ())), preferred_element_type=F32)


def hops(o):
    return min(o[0], NZ - o[0]) + min(o[1], NY - o[1])


OFFSETS = [(dz, dy) for dz in range(NZ) for dy in range(NY)]
NEAREST = sorted(OFFSETS, key=lambda o: (hops(o), o[1], o[0]))
PLANES = (4, 3, 5, 2, 6, 1, 7, 0)
LAST = 2
LAST_RELS = tuple(r for r in range(RELS) if RELATION_SOURCE[r] == LAST)


def kernel(feat_h, w_h, own_h, row_h, esrc_h, edst_h, ecnt_h, out,
           feat, w, own, row, esrc, edst, ecnt,
           rq, req_out, req_in, send, recv, lk, pc, plo, lohot, counts, deg, msgs, wt,
           gath, psend, precv, ins, rs, rr, ss, sr, lr, ps, pr):
    me, mm = lax.axis_index("dp"), lax.axis_index("mp")
    z, y = me // NY, me % NY
    n_mp = precv.shape[0]

    def fwd(o):
        return ((z + o[0]) % NZ) * NY + (y + o[1]) % NY

    def bwd(o):
        return ((z + NZ - o[0]) % NZ) * NY + (y + NY - o[1]) % NY

    groups = [NEAREST[4 * g:4 * g + 4] for g in range(8)]
    batch = {o: g for g in range(8) for o in groups[g]}

    def many(src, dst, send_sem, recv_sem):
        return pltpu.make_async_remote_copy(
            src, dst, send_sem, recv_sem, device_id={"dp": fwd((0, 1))}, device_id_type=MESH)

    barrier = pltpu.get_barrier_semaphore()
    for o in NEAREST[:0:-1]:
        pl.semaphore_signal(barrier, 1, device_id={"dp": fwd(o)}, device_id_type=MESH)
    for d in range(1, n_mp):
        pl.semaphore_signal(barrier, 1, device_id={"mp": (mm + d) % n_mp}, device_id_type=MESH)

    loads = [
        pltpu.make_async_copy(src, dst, ins.at[i])
        for i, (src, dst) in enumerate((
            (own_h, own), (row_h, row), (feat_h, feat), (esrc_h, esrc), (edst_h, edst),
            (ecnt_h, ecnt), (w_h, w)))
    ]
    for load in loads:
        load.start()

    upper = (iota((256, 256), 0) <= iota((256, 256), 1)).astype(F32).astype(BF16)
    base = jnp.zeros((TYPES * DP, 1), F32)
    acc = [jnp.zeros((2 * DP, CAP), F32) for _ in range(TYPES)]
    loads[0].wait()
    loads[1].wait()
    for blk in range(8):
        lanes = slice(blk * 256, (blk + 1) * 256)
        owners = [own[t, :, lanes] for t in range(TYPES)]
        ohs = [(iota((DP, 256), 0) == owners[t]).astype(F32) for t in range(TYPES)]
        oh = jnp.concatenate(ohs, axis=0)
        incl = dot(oh.astype(BF16), upper) + base
        base = incl[:, 255:256]
        ranked = oh * (incl - 1.0)
        for t in range(TYPES):
            rank = jnp.sum(ranked[t * DP:(t + 1) * DP], axis=0, keepdims=True).astype(I32)
            ids = row[t:t + 1, lanes]
            left = jnp.concatenate(
                [ohs[t] * (ids >> 8).astype(F32), ohs[t] * (ids & 255).astype(F32)], axis=0
            ).astype(BF16)
            acc[t] = acc[t] + dot_nt(left, hot(rank, CAP))
            lk[t, blk:blk + 1, :] = (owners[t] >> 1).astype(F32)
            lk[t, 8 + blk:9 + blk, :] = ((owners[t] & 1) * CAP + rank).astype(F32)
    for t in range(TYPES):
        rq[t * DP:(t + 1) * DP, :] = (acc[t][:DP] * 256.0 + acc[t][DP:]).astype(I32)
    for o in range(DP):
        req_out[o, :, :] = rq[pl.ds(o, TYPES, stride=DP), :]

    pl.semaphore_wait(barrier, DP - 1 + n_mp - 1)

    def req_copy(o):
        return pltpu.make_async_remote_copy(
            req_out.at[fwd(o)], req_in.at[me], rs.at[0], rr.at[batch[o]],
            device_id={"dp": fwd(o)}, device_id_type=MESH)

    for o in NEAREST[:0:-1]:
        req_copy(o).start()
    req_in[me] = req_out[me]

    def row_copy(t, o):
        return pltpu.make_async_remote_copy(
            send.at[t, bwd(o)], recv.at[t, me], ss.at[t],
            lr.at[o[0]] if t == LAST else sr.at[t],
            device_id={"dp": bwd(o)}, device_id_type=MESH)

    asked = set()

    def serve(t, group):
        for g in sorted({batch[o] for o in group} - asked):
            n = 3 if g == 0 else 4
            many(req_out.at[0:n], req_in.at[0:n], rs.at[0], rr.at[g]).wait_recv()
            asked.add(g)
        peers = [bwd(o) for o in group]
        ids = jnp.concatenate([req_in[p, t:t + 1, :] for p in peers], axis=1)
        low, high = ids & 255, ids >> 8
        table = jnp.concatenate([feat[t, :, c * 256:(c + 1) * 256] for c in range(8)], axis=0)
        res = dot(table, hot(low, 256))
        picked = res[0:64]
        for c in range(1, 8):
            picked = jnp.where(high == c, res[c * 64:(c + 1) * 64], picked)
        picked = picked.astype(BF16)
        for j, o in enumerate(group):
            piece = picked[:, j * CAP:(j + 1) * CAP]
            if o == (0, 0):
                recv[t, me] = piece
            else:
                send[t, peers[j]] = piece
        for o in group:
            if o != (0, 0):
                row_copy(t, o).start()

    loads[2].wait()
    for g in groups[:4]:
        serve(0, g)
        serve(1, g)
    for t in range(LAST):
        for g in groups[4:]:
            serve(t, g)
    for dz in PLANES:
        serve(LAST, [(dz, dy) for dy in range(NY)])

    loads[3].wait()
    for r in LAST_RELS:
        t = LAST

        def look(k, _, r=r, t=t):
            lanes = pl.ds(pl.multiple_of(k * EB, EB), EB)
            src = esrc[r:r + 1, lanes]
            res = dot(lk[t].astype(BF16), hot(src & 255, 256))
            here = iota((8, EB), 0) == (src >> 8)
            pc[r:r + 1, lanes] = jnp.sum(jnp.where(here, res[:8], 0.0), axis=0, keepdims=True)
            plo[r:r + 1, lanes] = jnp.sum(jnp.where(here, res[8:], 0.0), axis=0, keepdims=True)
            return 0

        lax.fori_loop(0, 2048 // EB, look, 0)
    loads[4].wait()
    loads[5].wait()
    loads[6].wait()

    for i, r in enumerate(LAST_RELS):
        slot = iota((1, 2048), 1)
        target = jnp.where(slot < ecnt[0, r], edst[r:r + 1, :], -1)
        deg[i] = dot_nt(jnp.ones((16, 2048), BF16), hot(target, SEEDS))
        lohot[...] = hot(plo[r:r + 1, :].astype(I32), 256)

        def count(n, _, i=i, r=r):
            slot = iota((1, 2048), 1)
            pair_id = jnp.where(slot < ecnt[0, r],
                                pc[r:r + 1, :].astype(I32) * SEEDS + edst[r:r + 1, :] - n * 256, -1)
            res = dot_nt(lohot[...], hot(pair_id, 256)).astype(BF16)
            counts[2 * n, :, i * SEEDS:(i + 1) * SEEDS] = res[:, :SEEDS]
            counts[2 * n + 1, :, i * SEEDS:(i + 1) * SEEDS] = res[:, SEEDS:]
            return 0

        lax.fori_loop(0, 8, count, 0)
    for c in range(16):
        seed = jnp.where(lk[LAST, 0:1, 0:SEEDS] == float(c), lk[LAST, 8:9, 0:SEEDS], -1.0)
        counts[c, :, 256:384] = hot(seed.astype(I32), 256)

    for a in range(TYPES):
        mats = [w[m].astype(F32) for m in STACKS[a]]
        if len(mats) < 4:
            mats.append(jnp.zeros_like(mats[0]))
            msgs[a, 192:256, :] = jnp.zeros((64, SEEDS), BF16)
        wt[a] = jnp.concatenate(mats, axis=0).T.astype(BF16)

    def landed(t, c):
        return jnp.concatenate([recv[t, 2 * c], recv[t, 2 * c + 1]], axis=1)

    def select(oh, chunk, parts):
        picked = None
        for g in range(0, len(parts), 4):
            res = dot(jnp.concatenate([part() for part in parts[g:g + 4]], axis=0), oh)
            for k in range(4):
                part = res[k * 64:(k + 1) * 64]
                picked = part if picked is None else jnp.where(chunk == g + k, part, picked)
        return picked.astype(BF16)

    def put(m, value):
        for a in range(TYPES):
            if m in STACKS[a]:
                k = STACKS[a].index(m) * 64
                msgs[a, k:k + 64, :] = value.astype(BF16)

    def all_rows(t, sems):
        return many(send.at[t, 0:DP - 1], recv.at[t, 0:DP - 1], ss.at[t], sems)

    many(req_out.at[0:DP - 1], req_in.at[0:DP - 1], rs.at[0], rr.at[0]).wait_send()
    for t in range(LAST):
        all_rows(t, sr.at[t]).wait_recv()

        def gather(k, _, t=t):
            chunk, low = (
                jnp.concatenate([lk[t, pl.ds(b + 2 * k, 1), :], lk[t, pl.ds(b + 2 * k + 1, 1), :]],
                                axis=1).astype(I32) for b in (0, 8))
            gath[:, pl.ds(pl.multiple_of(k * EB, EB), EB)] = select(
                hot(low, 256), chunk, [lambda c=c: landed(t, c) for c in range(16)])
            return 0

        lax.fori_loop(0, 2048 // EB, gather, 0)
        put(RELS + t, gath[:, 0:SEEDS])
        for r in range(RELS):
            if RELATION_SOURCE[r] != t:
                continue
            live = ecnt[0, r]

            def edges(k, total, r=r, live=live):
                lanes = pl.ds(pl.multiple_of(k * EB, EB), EB)
                src = esrc[r:r + 1, lanes]
                rows = select(hot(src & 255, 256), src >> 8,
                              [lambda c=c: gath[:, c * 256:(c + 1) * 256] for c in range(8)])
                rows = jnp.concatenate([rows, jnp.ones((16, EB), BF16)], axis=0)
                slot = iota((1, EB), 1) + k * EB
                target = jnp.where(slot < live, edst[r:r + 1, lanes], -1)
                return total + dot_nt(rows, hot(target, SEEDS))

            total = lax.fori_loop(0, 2048 // EB, edges, jnp.zeros((80, SEEDS), F32))
            put(r, total[:64] / jnp.maximum(total[64:65], 1.0))
        all_rows(t, sr.at[t]).wait_send()

    total = jnp.zeros((64, 384), F32)
    for dz in PLANES:
        n = NY - 1 if dz == 0 else NY
        many(send.at[LAST, 0:n], recv.at[LAST, 0:n], ss.at[LAST], lr.at[dz]).wait_recv()
        for h in range(2):
            c = ((z + dz) % NZ) * 2 + h
            total = total + dot(landed(LAST, c), counts[c])
    for i, r in enumerate(LAST_RELS):
        put(r, total[:, i * SEEDS:(i + 1) * SEEDS] / jnp.maximum(deg[i, 0:1, :], 1.0))
    put(RELS + LAST, total[:, 256:384])

    def part_copy(d):
        p = (mm + d) % n_mp
        return pltpu.make_async_remote_copy(
            psend.at[p], precv.at[mm], ps.at[0], pr.at[0],
            device_id={"mp": p}, device_id_type=MESH)

    for a in range(TYPES):
        part = dot(wt[a], msgs[a]).astype(BF16)
        for p in range(n_mp):
            psend[p, a] = part[p * 64:(p + 1) * 64]
    for d in (4, 3, 5, 2, 6, 1, 7):
        part_copy(d).start()
    precv[mm] = psend[mm]
    all_rows(LAST, sr.at[0]).wait_send()
    many(psend.at[0:n_mp - 1], precv.at[0:n_mp - 1], ps.at[0], pr.at[0]).wait_recv()
    for a in range(TYPES):
        typed = precv[0, a].astype(F32)
        for p in range(1, n_mp):
            typed = typed + precv[p, a].astype(F32)
        out[a] = jnp.maximum(typed, 0.0).astype(BF16)
    many(psend.at[0:n_mp - 1], precv.at[0:n_mp - 1], ps.at[0], pr.at[0]).wait_send()


def solution(mesh):
    n_mp = mesh.shape["mp"]

    def per_device(features, weights, sample_owner, sample_row, edge_src, edge_dst, edge_count):
        return pl.pallas_call(
            kernel,
            out_shape=pltpu.VMEM((TYPES, 64, SEEDS), BF16),
            in_specs=[pl.BlockSpec(memory_space=pltpu.HBM)] * 7,
            out_specs=pl.BlockSpec(memory_space=pltpu.VMEM),
            scratch_shapes=[
                pltpu.VMEM((TYPES, 64, 2048), BF16),
                pltpu.VMEM((11, 64, 512), BF16),
                pltpu.VMEM((TYPES, 1, 2048), I32),
                pltpu.VMEM((TYPES, 2048), I32),
                pltpu.VMEM((RELS, 2048), I32),
                pltpu.VMEM((RELS, 2048), I32),
                pltpu.SMEM((1, RELS), I32),
                pltpu.VMEM((TYPES * DP, CAP), I32),
                pltpu.VMEM((DP, TYPES, CAP), I32),
                pltpu.VMEM((DP, TYPES, CAP), I32),
                pltpu.VMEM((TYPES, DP, 64, CAP), BF16),
                pltpu.VMEM((TYPES, DP, 64, CAP), BF16),
                pltpu.VMEM((TYPES, 16, 256), F32),
                pltpu.VMEM((RELS, 2048), F32),
                pltpu.VMEM((RELS, 2048), F32),
                pltpu.VMEM((256, 2048), BF16),
                pltpu.VMEM((16, 256, 384), BF16),
                pltpu.VMEM((len(LAST_RELS), 16, SEEDS), F32),
                pltpu.VMEM((TYPES, 256, SEEDS), BF16),
                pltpu.VMEM((TYPES, 512, 256), BF16),
                pltpu.VMEM((64, 2048), BF16),
                pltpu.VMEM((n_mp, TYPES, 64, SEEDS), BF16),
                pltpu.VMEM((n_mp, TYPES, 64, SEEDS), BF16),
                pltpu.SemaphoreType.DMA((7,)),
                pltpu.SemaphoreType.DMA((1,)),
                pltpu.SemaphoreType.DMA((8,)),
                pltpu.SemaphoreType.DMA((TYPES,)),
                pltpu.SemaphoreType.DMA((LAST,)),
                pltpu.SemaphoreType.DMA((NZ,)),
                pltpu.SemaphoreType.DMA((1,)),
                pltpu.SemaphoreType.DMA((1,)),
            ],
            compiler_params=pltpu.CompilerParams(
                collective_id=0, has_side_effects=True, vmem_limit_bytes=60000000),
        )(features, weights, jnp.transpose(sample_owner, (0, 2, 1)), sample_row,
          edge_src, edge_dst, jnp.transpose(edge_count, (1, 0)))

    return jax.shard_map(
        per_device,
        mesh=mesh,
        in_specs=(
            P(None, "mp", "dp"),
            P(None, "mp", None),
            P(None, "dp", None),
            P(None, "dp"),
            P(None, "dp"),
            P(None, "dp"),
            P(None, "dp"),
        ),
        out_specs=P(None, "mp", "dp"),
        check_vma=False,
    )
```

```python
import jax
import jax.numpy as jnp
from jax import lax
from jax.experimental import pallas as pl
from jax.experimental.pallas import tpu as pltpu
from jax.sharding import PartitionSpec as P

TYPES = 3
RELS = 8
SEEDS = 128
CAP = 128
RELATION_SOURCE = (0, 1, 0, 1, 2, 0, 2, 1)
STACKS = ((1, 2, 6, 8), (0, 4, 7, 9), (3, 5, 10))
NZ, NY = 8, 4
DP = NZ * NY
MESH = pl.DeviceIdType.MESH
F32, BF16, I32 = jnp.float32, jnp.bfloat16, jnp.int32
EB = 512


def iota(shape, dim):
    return lax.broadcasted_iota(I32, shape, dim)


def hot(ids, rows):
    return (iota((rows, ids.shape[1]), 0) == ids).astype(F32).astype(BF16)


def dot(a, b):
    return jnp.dot(a, b, preferred_element_type=F32)


def dot_nt(a, b):
    return lax.dot_general(a, b, (((1,), (1,)), ((), ())), preferred_element_type=F32)


def hops(o):
    return min(o[0], NZ - o[0]) + min(o[1], NY - o[1])


OFFSETS = [(dz, dy) for dz in range(NZ) for dy in range(NY)]
NEAREST = sorted(OFFSETS, key=lambda o: (hops(o), o[1], o[0]))
PLANES = (4, 3, 5, 2, 6, 1, 7, 0)
LAST = 2
LAST_RELS = tuple(r for r in range(RELS) if RELATION_SOURCE[r] == LAST)


def kernel(feat_h, w_h, own_h, row_h, esrc_h, edst_h, ecnt_h, out,
           feat, w, own, row, esrc, edst, ecnt,
           rq, req_out, req_in, send, recv, lk, pc, plo, lohot, counts, deg, msgs, wt,
           gath, psend, precv, pair, comb, ins, rs, rr, ss, sr, lr, ps, pr):
    me, mm = lax.axis_index("dp"), lax.axis_index("mp")
    z, y = me // NY, me % NY
    n_mp = precv.shape[0]
    nx = n_mp // 2
    x, core = mm // 2, mm % 2
    sibling = x * 2 + (1 - core)
    opposite = ((x + 2) % nx) * 2 + core
    beside = [((x + d) % nx) * 2 + k for d in (1, nx - 1) for k in range(2)]

    def fwd(o):
        return ((z + o[0]) % NZ) * NY + (y + o[1]) % NY

    def bwd(o):
        return ((z + NZ - o[0]) % NZ) * NY + (y + NY - o[1]) % NY

    groups = [NEAREST[4 * g:4 * g + 4] for g in range(8)]
    batch = {o: g for g in range(8) for o in groups[g]}

    def many(src, dst, send_sem, recv_sem):
        return pltpu.make_async_remote_copy(
            src, dst, send_sem, recv_sem, device_id={"dp": fwd((0, 1))}, device_id_type=MESH)

    barrier = pltpu.get_barrier_semaphore()
    for o in NEAREST[:0:-1]:
        pl.semaphore_signal(barrier, 1, device_id={"dp": fwd(o)}, device_id_type=MESH)
    for p in [opposite] + beside + [sibling]:
        pl.semaphore_signal(barrier, 1, device_id={"mp": p}, device_id_type=MESH)

    loads = [
        pltpu.make_async_copy(src, dst, ins.at[i])
        for i, (src, dst) in enumerate((
            (own_h, own), (row_h, row), (feat_h, feat), (esrc_h, esrc), (edst_h, edst),
            (ecnt_h, ecnt), (w_h, w)))
    ]
    for load in loads:
        load.start()

    upper = (iota((256, 256), 0) <= iota((256, 256), 1)).astype(F32).astype(BF16)
    base = jnp.zeros((TYPES * DP, 1), F32)
    acc = [jnp.zeros((2 * DP, CAP), F32) for _ in range(TYPES)]
    loads[0].wait()
    loads[1].wait()
    for blk in range(8):
        lanes = slice(blk * 256, (blk + 1) * 256)
        owners = [own[t, :, lanes] for t in range(TYPES)]
        ohs = [(iota((DP, 256), 0) == owners[t]).astype(F32) for t in range(TYPES)]
        oh = jnp.concatenate(ohs, axis=0)
        incl = dot(oh.astype(BF16), upper) + base
        base = incl[:, 255:256]
        ranked = oh * (incl - 1.0)
        for t in range(TYPES):
            rank = jnp.sum(ranked[t * DP:(t + 1) * DP], axis=0, keepdims=True).astype(I32)
            ids = row[t:t + 1, lanes]
            left = jnp.concatenate(
                [ohs[t] * (ids >> 8).astype(F32), ohs[t] * (ids & 255).astype(F32)], axis=0
            ).astype(BF16)
            acc[t] = acc[t] + dot_nt(left, hot(rank, CAP))
            lk[t, blk:blk + 1, :] = (owners[t] >> 1).astype(F32)
            lk[t, 8 + blk:9 + blk, :] = ((owners[t] & 1) * CAP + rank).astype(F32)
    for t in range(TYPES):
        rq[t * DP:(t + 1) * DP, :] = (acc[t][:DP] * 256.0 + acc[t][DP:]).astype(I32)
    for o in range(DP):
        req_out[o, :, :] = rq[pl.ds(o, TYPES, stride=DP), :]

    pl.semaphore_wait(barrier, DP - 1 + 6)

    def req_copy(o):
        return pltpu.make_async_remote_copy(
            req_out.at[fwd(o)], req_in.at[me], rs.at[0], rr.at[batch[o]],
            device_id={"dp": fwd(o)}, device_id_type=MESH)

    for o in NEAREST[1:]:
        req_copy(o).start()
    req_in[me] = req_out[me]

    def row_copy(t, o):
        return pltpu.make_async_remote_copy(
            send.at[t, bwd(o)], recv.at[t, me], ss.at[t],
            lr.at[o[0]] if t == LAST else sr.at[t],
            device_id={"dp": bwd(o)}, device_id_type=MESH)

    asked = set()

    def serve(t, group):
        for g in sorted({batch[o] for o in group} - asked):
            n = 3 if g == 0 else 4
            many(req_out.at[0:n], req_in.at[0:n], rs.at[0], rr.at[g]).wait_recv()
            asked.add(g)
        peers = [bwd(o) for o in group]
        ids = jnp.concatenate([req_in[p, t:t + 1, :] for p in peers], axis=1)
        low, high = ids & 255, ids >> 8
        table = jnp.concatenate([feat[t, :, c * 256:(c + 1) * 256] for c in range(8)], axis=0)
        res = dot(table, hot(low, 256))
        picked = res[0:64]
        for c in range(1, 8):
            picked = jnp.where(high == c, res[c * 64:(c + 1) * 64], picked)
        picked = picked.astype(BF16)
        for j, o in enumerate(group):
            piece = picked[:, j * CAP:(j + 1) * CAP]
            if o == (0, 0):
                recv[t, me] = piece
            else:
                send[t, peers[j]] = piece
        for o in group:
            if o != (0, 0):
                row_copy(t, o).start()

    loads[2].wait()
    for g in groups[:4]:
        serve(0, g)
        serve(1, g)
    for t in range(LAST):
        for g in groups[4:]:
            serve(t, g)
    for dz in PLANES:
        serve(LAST, [(dz, dy) for dy in range(NY)])

    loads[3].wait()
    for r in LAST_RELS:
        t = LAST

        def look(k, _, r=r, t=t):
            lanes = pl.ds(pl.multiple_of(k * EB, EB), EB)
            src = esrc[r:r + 1, lanes]
            res = dot(lk[t].astype(BF16), hot(src & 255, 256))
            here = iota((8, EB), 0) == (src >> 8)
            pc[r:r + 1, lanes] = jnp.sum(jnp.where(here, res[:8], 0.0), axis=0, keepdims=True)
            plo[r:r + 1, lanes] = jnp.sum(jnp.where(here, res[8:], 0.0), axis=0, keepdims=True)
            return 0

        lax.fori_loop(0, 2048 // EB, look, 0)
    loads[4].wait()
    loads[5].wait()
    loads[6].wait()

    for i, r in enumerate(LAST_RELS):
        slot = iota((1, 2048), 1)
        target = jnp.where(slot < ecnt[0, r], edst[r:r + 1, :], -1)
        deg[i] = dot_nt(jnp.ones((16, 2048), BF16), hot(target, SEEDS))
        lohot[...] = hot(plo[r:r + 1, :].astype(I32), 256)

        def count(n, _, i=i, r=r):
            slot = iota((1, 2048), 1)
            pair_id = jnp.where(slot < ecnt[0, r],
                                pc[r:r + 1, :].astype(I32) * SEEDS + edst[r:r + 1, :] - n * 256, -1)
            res = dot_nt(lohot[...], hot(pair_id, 256)).astype(BF16)
            counts[2 * n, :, i * SEEDS:(i + 1) * SEEDS] = res[:, :SEEDS]
            counts[2 * n + 1, :, i * SEEDS:(i + 1) * SEEDS] = res[:, SEEDS:]
            return 0

        lax.fori_loop(0, 8, count, 0)
    for c in range(16):
        seed = jnp.where(lk[LAST, 0:1, 0:SEEDS] == float(c), lk[LAST, 8:9, 0:SEEDS], -1.0)
        counts[c, :, 256:384] = hot(seed.astype(I32), 256)

    for a in range(TYPES):
        mats = [w[m].astype(F32) for m in STACKS[a]]
        if len(mats) < 4:
            mats.append(jnp.zeros_like(mats[0]))
            msgs[a, 192:256, :] = jnp.zeros((64, SEEDS), BF16)
        wt[a] = jnp.concatenate(mats, axis=0).T.astype(BF16)

    def landed(t, c):
        return jnp.concatenate([recv[t, 2 * c], recv[t, 2 * c + 1]], axis=1)

    def select(oh, chunk, parts):
        picked = None
        for g in range(0, len(parts), 4):
            res = dot(jnp.concatenate([part() for part in parts[g:g + 4]], axis=0), oh)
            for k in range(4):
                part = res[k * 64:(k + 1) * 64]
                picked = part if picked is None else jnp.where(chunk == g + k, part, picked)
        return picked.astype(BF16)

    def put(m, value):
        for a in range(TYPES):
            if m in STACKS[a]:
                k = STACKS[a].index(m) * 64
                msgs[a, k:k + 64, :] = value.astype(BF16)

    def all_rows(t, sems):
        return many(send.at[t, 0:DP - 1], recv.at[t, 0:DP - 1], ss.at[t], sems)

    many(req_out.at[0:DP - 1], req_in.at[0:DP - 1], rs.at[0], rr.at[0]).wait_send()
    for t in range(LAST):
        all_rows(t, sr.at[t]).wait_recv()

        def gather(k, _, t=t):
            chunk, low = (
                jnp.concatenate([lk[t, pl.ds(b + 2 * k, 1), :], lk[t, pl.ds(b + 2 * k + 1, 1), :]],
                                axis=1).astype(I32) for b in (0, 8))
            gath[:, pl.ds(pl.multiple_of(k * EB, EB), EB)] = select(
                hot(low, 256), chunk, [lambda c=c: landed(t, c) for c in range(16)])
            return 0

        lax.fori_loop(0, 2048 // EB, gather, 0)
        put(RELS + t, gath[:, 0:SEEDS])
        for r in range(RELS):
            if RELATION_SOURCE[r] != t:
                continue
            live = ecnt[0, r]

            def edges(k, total, r=r, live=live):
                lanes = pl.ds(pl.multiple_of(k * EB, EB), EB)
                src = esrc[r:r + 1, lanes]
                rows = select(hot(src & 255, 256), src >> 8,
                              [lambda c=c: gath[:, c * 256:(c + 1) * 256] for c in range(8)])
                rows = jnp.concatenate([rows, jnp.ones((16, EB), BF16)], axis=0)
                slot = iota((1, EB), 1) + k * EB
                target = jnp.where(slot < live, edst[r:r + 1, lanes], -1)
                return total + dot_nt(rows, hot(target, SEEDS))

            total = lax.fori_loop(0, 2048 // EB, edges, jnp.zeros((80, SEEDS), F32))
            put(r, total[:64] / jnp.maximum(total[64:65], 1.0))
        all_rows(t, sr.at[t]).wait_send()

    total = jnp.zeros((64, 384), F32)
    for dz in PLANES:
        n = NY - 1 if dz == 0 else NY
        many(send.at[LAST, 0:n], recv.at[LAST, 0:n], ss.at[LAST], lr.at[dz]).wait_recv()
        for h in range(2):
            c = ((z + dz) % NZ) * 2 + h
            total = total + dot(landed(LAST, c), counts[c])
    for i, r in enumerate(LAST_RELS):
        put(r, total[:, i * SEEDS:(i + 1) * SEEDS] / jnp.maximum(deg[i, 0:1, :], 1.0))
    put(RELS + LAST, total[:, 256:384])

    def part_copy(p):
        return pltpu.make_async_remote_copy(
            psend.at[p], precv.at[mm], ps.at[0], pr.at[0],
            device_id={"mp": p}, device_id_type=MESH)

    pair_copy = pltpu.make_async_remote_copy(
        psend.at[((x + 2) % nx) * 2 + (1 - core)], pair, ps.at[1], pr.at[1],
        device_id={"mp": sibling}, device_id_type=MESH)
    far_copy = pltpu.make_async_remote_copy(
        comb, precv.at[mm], ps.at[2], pr.at[2], device_id={"mp": opposite}, device_id_type=MESH)

    for a in range(TYPES):
        part = dot(wt[a], msgs[a]).astype(BF16)
        for p in range(n_mp):
            psend[p, a] = part[p * 64:(p + 1) * 64]
    pair_copy.start()
    for p in beside:
        part_copy(p).start()
    part_copy(sibling).start()
    pair_copy.wait_recv()
    comb[...] = (psend[opposite].astype(F32) + pair[...].astype(F32)).astype(BF16)
    far_copy.start()
    all_rows(LAST, sr.at[0]).wait_send()
    many(psend.at[0:5], precv.at[0:5], ps.at[0], pr.at[0]).wait_recv()
    typed = psend[mm].astype(F32)
    for p in beside + [sibling]:
        typed = typed + precv[p].astype(F32)
    far_copy.wait_recv()
    out[...] = jnp.maximum(typed + precv[opposite].astype(F32), 0.0).astype(BF16)
    many(psend.at[0:5], precv.at[0:5], ps.at[0], pr.at[0]).wait_send()
    pair_copy.wait_send()
    far_copy.wait_send()


def solution(mesh):
    n_mp = mesh.shape["mp"]

    def per_device(features, weights, sample_owner, sample_row, edge_src, edge_dst, edge_count):
        return pl.pallas_call(
            kernel,
            out_shape=pltpu.VMEM((TYPES, 64, SEEDS), BF16),
            in_specs=[pl.BlockSpec(memory_space=pltpu.HBM)] * 7,
            out_specs=pl.BlockSpec(memory_space=pltpu.VMEM),
            scratch_shapes=[
                pltpu.VMEM((TYPES, 64, 2048), BF16),
                pltpu.VMEM((11, 64, 512), BF16),
                pltpu.VMEM((TYPES, 1, 2048), I32),
                pltpu.VMEM((TYPES, 2048), I32),
                pltpu.VMEM((RELS, 2048), I32),
                pltpu.VMEM((RELS, 2048), I32),
                pltpu.SMEM((1, RELS), I32),
                pltpu.VMEM((TYPES * DP, CAP), I32),
                pltpu.VMEM((DP, TYPES, CAP), I32),
                pltpu.VMEM((DP, TYPES, CAP), I32),
                pltpu.VMEM((TYPES, DP, 64, CAP), BF16),
                pltpu.VMEM((TYPES, DP, 64, CAP), BF16),
                pltpu.VMEM((TYPES, 16, 256), F32),
                pltpu.VMEM((RELS, 2048), F32),
                pltpu.VMEM((RELS, 2048), F32),
                pltpu.VMEM((256, 2048), BF16),
                pltpu.VMEM((16, 256, 384), BF16),
                pltpu.VMEM((len(LAST_RELS), 16, SEEDS), F32),
                pltpu.VMEM((TYPES, 256, SEEDS), BF16),
                pltpu.VMEM((TYPES, 512, 256), BF16),
                pltpu.VMEM((64, 2048), BF16),
                pltpu.VMEM((n_mp, TYPES, 64, SEEDS), BF16),
                pltpu.VMEM((n_mp, TYPES, 64, SEEDS), BF16),
                pltpu.VMEM((TYPES, 64, SEEDS), BF16),
                pltpu.VMEM((TYPES, 64, SEEDS), BF16),
                pltpu.SemaphoreType.DMA((7,)),
                pltpu.SemaphoreType.DMA((1,)),
                pltpu.SemaphoreType.DMA((8,)),
                pltpu.SemaphoreType.DMA((TYPES,)),
                pltpu.SemaphoreType.DMA((LAST,)),
                pltpu.SemaphoreType.DMA((NZ,)),
                pltpu.SemaphoreType.DMA((3,)),
                pltpu.SemaphoreType.DMA((3,)),
            ],
            compiler_params=pltpu.CompilerParams(
                collective_id=0, has_side_effects=True, vmem_limit_bytes=60000000),
        )(features, weights, jnp.transpose(sample_owner, (0, 2, 1)), sample_row,
          edge_src, edge_dst, jnp.transpose(edge_count, (1, 0)))

    return jax.shard_map(
        per_device,
        mesh=mesh,
        in_specs=(
            P(None, "mp", "dp"),
            P(None, "mp", None),
            P(None, "dp", None),
            P(None, "dp"),
            P(None, "dp"),
            P(None, "dp"),
            P(None, "dp"),
        ),
        out_specs=P(None, "mp", "dp"),
        check_vma=False,
    )
```

```python
import jax
import jax.numpy as jnp
from jax import lax
from jax.experimental import pallas as pl
from jax.experimental.pallas import tpu as pltpu
from jax.sharding import PartitionSpec as P

TYPES = 3
RELS = 8
SEEDS = 128
CAP = 128
RELATION_SOURCE = (0, 1, 0, 1, 2, 0, 2, 1)
STACKS = ((1, 2, 6, 8), (0, 4, 7, 9), (3, 5, 10))
NZ, NY = 8, 4
DP = NZ * NY
MESH = pl.DeviceIdType.MESH
F32, BF16, I32 = jnp.float32, jnp.bfloat16, jnp.int32
EB = 512


def iota(shape, dim):
    return lax.broadcasted_iota(I32, shape, dim)


def hot(ids, rows):
    return (iota((rows, ids.shape[1]), 0) == ids).astype(F32).astype(BF16)


def dot(a, b):
    return jnp.dot(a, b, preferred_element_type=F32)


def dot_nt(a, b):
    return lax.dot_general(a, b, (((1,), (1,)), ((), ())), preferred_element_type=F32)


def hops(o):
    return min(o[0], NZ - o[0]) + min(o[1], NY - o[1])


OFFSETS = [(dz, dy) for dz in range(NZ) for dy in range(NY)]
NEAREST = sorted(OFFSETS, key=lambda o: (hops(o), o[1], o[0]))
PLANES = (4, 3, 5, 2, 6, 1, 7, 0)
LAST = 2
LAST_RELS = tuple(r for r in range(RELS) if RELATION_SOURCE[r] == LAST)


def kernel(feat_h, w_h, own_h, row_h, esrc_h, edst_h, ecnt_h, out,
           feat, w, own, row, esrc, edst, ecnt,
           rq, req_out, req_in, send, recv, lk, pc, plo, lohot, counts, deg, msgs, wt,
           gath, psend, precv, ins, rs, rr, ss, sr, lr, ps, pr):
    me, mm = lax.axis_index("dp"), lax.axis_index("mp")
    z, y = me // NY, me % NY
    n_mp = precv.shape[0]

    def fwd(o):
        return ((z + o[0]) % NZ) * NY + (y + o[1]) % NY

    def bwd(o):
        return ((z + NZ - o[0]) % NZ) * NY + (y + NY - o[1]) % NY

    groups = [NEAREST[4 * g:4 * g + 4] for g in range(8)]
    batch = {o: g for g in range(8) for o in groups[g]}

    def many(src, dst, send_sem, recv_sem):
        return pltpu.make_async_remote_copy(
            src, dst, send_sem, recv_sem, device_id={"dp": fwd((0, 1))}, device_id_type=MESH)

    barrier = pltpu.get_barrier_semaphore()
    for o in NEAREST[:0:-1]:
        pl.semaphore_signal(barrier, 1, device_id={"dp": fwd(o)}, device_id_type=MESH)
    for d in range(1, n_mp):
        pl.semaphore_signal(barrier, 1, device_id={"mp": (mm + d) % n_mp}, device_id_type=MESH)

    loads = [
        pltpu.make_async_copy(src, dst, ins.at[i])
        for i, (src, dst) in enumerate((
            (own_h, own), (row_h, row), (feat_h, feat), (esrc_h, esrc), (edst_h, edst),
            (ecnt_h, ecnt), (w_h, w)))
    ]
    for load in loads:
        load.start()

    upper = (iota((256, 256), 0) <= iota((256, 256), 1)).astype(F32).astype(BF16)
    base = jnp.zeros((TYPES * DP, 1), F32)
    acc = [jnp.zeros((2 * DP, CAP), F32) for _ in range(TYPES)]
    loads[0].wait()
    loads[1].wait()
    for blk in range(8):
        lanes = slice(blk * 256, (blk + 1) * 256)
        owners = [own[t, :, lanes] for t in range(TYPES)]
        ohs = [(iota((DP, 256), 0) == owners[t]).astype(F32) for t in range(TYPES)]
        oh = jnp.concatenate(ohs, axis=0)
        incl = dot(oh.astype(BF16), upper) + base
        base = incl[:, 255:256]
        ranked = oh * (incl - 1.0)
        for t in range(TYPES):
            rank = jnp.sum(ranked[t * DP:(t + 1) * DP], axis=0, keepdims=True).astype(I32)
            ids = row[t:t + 1, lanes]
            left = jnp.concatenate(
                [ohs[t] * (ids >> 8).astype(F32), ohs[t] * (ids & 255).astype(F32)], axis=0
            ).astype(BF16)
            acc[t] = acc[t] + dot_nt(left, hot(rank, CAP))
            lk[t, blk:blk + 1, :] = (owners[t] >> 1).astype(F32)
            lk[t, 8 + blk:9 + blk, :] = ((owners[t] & 1) * CAP + rank).astype(F32)
    for t in range(TYPES):
        rq[t * DP:(t + 1) * DP, :] = (acc[t][:DP] * 256.0 + acc[t][DP:]).astype(I32)
    for o in range(DP):
        req_out[o, :, :] = rq[pl.ds(o, TYPES, stride=DP), :]

    pl.semaphore_wait(barrier, DP - 1 + n_mp - 1)

    def req_copy(o):
        return pltpu.make_async_remote_copy(
            req_out.at[fwd(o)], req_in.at[me], rs.at[0], rr.at[batch[o]],
            device_id={"dp": fwd(o)}, device_id_type=MESH)

    for o in NEAREST[:0:-1]:
        req_copy(o).start()
    req_in[me] = req_out[me]

    def row_copy(t, o):
        return pltpu.make_async_remote_copy(
            send.at[t, bwd(o)], recv.at[t, me], ss.at[t],
            lr.at[o[0]] if t == LAST else sr.at[t],
            device_id={"dp": bwd(o)}, device_id_type=MESH)

    asked = set()

    def serve(t, group):
        for g in sorted({batch[o] for o in group} - asked):
            n = 3 if g == 0 else 4
            many(req_out.at[0:n], req_in.at[0:n], rs.at[0], rr.at[g]).wait_recv()
            asked.add(g)
        peers = [bwd(o) for o in group]
        ids = jnp.concatenate([req_in[p, t:t + 1, :] for p in peers], axis=1)
        low, high = ids & 255, ids >> 8
        table = jnp.concatenate([feat[t, :, c * 256:(c + 1) * 256] for c in range(8)], axis=0)
        res = dot(table, hot(low, 256))
        picked = res[0:64]
        for c in range(1, 8):
            picked = jnp.where(high == c, res[c * 64:(c + 1) * 64], picked)
        picked = picked.astype(BF16)
        for j, o in enumerate(group):
            piece = picked[:, j * CAP:(j + 1) * CAP]
            if o == (0, 0):
                recv[t, me] = piece
            else:
                send[t, peers[j]] = piece
        for o in group:
            if o != (0, 0):
                row_copy(t, o).start()

    loads[2].wait()
    for g in groups:
        serve(0, g)
        serve(1, g)
    for dz in PLANES:
        serve(LAST, [(dz, dy) for dy in range(NY)])

    loads[3].wait()
    for r in LAST_RELS:
        t = LAST

        def look(k, _, r=r, t=t):
            lanes = pl.ds(pl.multiple_of(k * EB, EB), EB)
            src = esrc[r:r + 1, lanes]
            res = dot(lk[t].astype(BF16), hot(src & 255, 256))
            here = iota((8, EB), 0) == (src >> 8)
            pc[r:r + 1, lanes] = jnp.sum(jnp.where(here, res[:8], 0.0), axis=0, keepdims=True)
            plo[r:r + 1, lanes] = jnp.sum(jnp.where(here, res[8:], 0.0), axis=0, keepdims=True)
            return 0

        lax.fori_loop(0, 2048 // EB, look, 0)
    loads[4].wait()
    loads[5].wait()
    loads[6].wait()

    for i, r in enumerate(LAST_RELS):
        slot = iota((1, 2048), 1)
        target = jnp.where(slot < ecnt[0, r], edst[r:r + 1, :], -1)
        deg[i] = dot_nt(jnp.ones((16, 2048), BF16), hot(target, SEEDS))
        lohot[...] = hot(plo[r:r + 1, :].astype(I32), 256)

        def count(n, _, i=i, r=r):
            slot = iota((1, 2048), 1)
            pair_id = jnp.where(slot < ecnt[0, r],
                                pc[r:r + 1, :].astype(I32) * SEEDS + edst[r:r + 1, :] - n * 256, -1)
            res = dot_nt(lohot[...], hot(pair_id, 256)).astype(BF16)
            counts[2 * n, :, i * SEEDS:(i + 1) * SEEDS] = res[:, :SEEDS]
            counts[2 * n + 1, :, i * SEEDS:(i + 1) * SEEDS] = res[:, SEEDS:]
            return 0

        lax.fori_loop(0, 8, count, 0)
    for c in range(16):
        seed = jnp.where(lk[LAST, 0:1, 0:SEEDS] == float(c), lk[LAST, 8:9, 0:SEEDS], -1.0)
        counts[c, :, 256:384] = hot(seed.astype(I32), 256)

    for a in range(TYPES):
        mats = [w[m].astype(F32) for m in STACKS[a]]
        if len(mats) < 4:
            mats.append(jnp.zeros_like(mats[0]))
            msgs[a, 192:256, :] = jnp.zeros((64, SEEDS), BF16)
        wt[a] = jnp.concatenate(mats, axis=0).T.astype(BF16)

    def landed(t, c):
        return jnp.concatenate([recv[t, 2 * c], recv[t, 2 * c + 1]], axis=1)

    def select(oh, chunk, parts):
        picked = None
        for g in range(0, len(parts), 4):
            res = dot(jnp.concatenate([part() for part in parts[g:g + 4]], axis=0), oh)
            for k in range(4):
                part = res[k * 64:(k + 1) * 64]
                picked = part if picked is None else jnp.where(chunk == g + k, part, picked)
        return picked.astype(BF16)

    def put(m, value):
        for a in range(TYPES):
            if m in STACKS[a]:
                k = STACKS[a].index(m) * 64
                msgs[a, k:k + 64, :] = value.astype(BF16)

    def all_rows(t, sems):
        return many(send.at[t, 0:DP - 1], recv.at[t, 0:DP - 1], ss.at[t], sems)

    many(req_out.at[0:DP - 1], req_in.at[0:DP - 1], rs.at[0], rr.at[0]).wait_send()
    for t in range(LAST):
        all_rows(t, sr.at[t]).wait_recv()

        def gather(k, _, t=t):
            chunk, low = (
                jnp.concatenate([lk[t, pl.ds(b + 2 * k, 1), :], lk[t, pl.ds(b + 2 * k + 1, 1), :]],
                                axis=1).astype(I32) for b in (0, 8))
            gath[:, pl.ds(pl.multiple_of(k * EB, EB), EB)] = select(
                hot(low, 256), chunk, [lambda c=c: landed(t, c) for c in range(16)])
            return 0

        lax.fori_loop(0, 2048 // EB, gather, 0)
        put(RELS + t, gath[:, 0:SEEDS])
        for r in range(RELS):
            if RELATION_SOURCE[r] != t:
                continue
            live = ecnt[0, r]

            def edges(k, total, r=r, live=live):
                lanes = pl.ds(pl.multiple_of(k * EB, EB), EB)
                src = esrc[r:r + 1, lanes]
                rows = select(hot(src & 255, 256), src >> 8,
                              [lambda c=c: gath[:, c * 256:(c + 1) * 256] for c in range(8)])
                rows = jnp.concatenate([rows, jnp.ones((16, EB), BF16)], axis=0)
                slot = iota((1, EB), 1) + k * EB
                target = jnp.where(slot < live, edst[r:r + 1, lanes], -1)
                return total + dot_nt(rows, hot(target, SEEDS))

            total = lax.fori_loop(0, 2048 // EB, edges, jnp.zeros((80, SEEDS), F32))
            put(r, total[:64] / jnp.maximum(total[64:65], 1.0))
        all_rows(t, sr.at[t]).wait_send()

    total = jnp.zeros((64, 384), F32)
    for dz in PLANES:
        n = NY - 1 if dz == 0 else NY
        many(send.at[LAST, 0:n], recv.at[LAST, 0:n], ss.at[LAST], lr.at[dz]).wait_recv()
        for h in range(2):
            c = ((z + dz) % NZ) * 2 + h
            total = total + dot(landed(LAST, c), counts[c])
    for i, r in enumerate(LAST_RELS):
        put(r, total[:, i * SEEDS:(i + 1) * SEEDS] / jnp.maximum(deg[i, 0:1, :], 1.0))
    put(RELS + LAST, total[:, 256:384])

    def part_copy(d):
        p = (mm + d) % n_mp
        return pltpu.make_async_remote_copy(
            psend.at[p], precv.at[mm], ps.at[0], pr.at[0],
            device_id={"mp": p}, device_id_type=MESH)

    for a in range(TYPES):
        part = dot(wt[a], msgs[a]).astype(BF16)
        for p in range(n_mp):
            psend[p, a] = part[p * 64:(p + 1) * 64]
    for d in (4, 3, 5, 2, 6, 1, 7):
        part_copy(d).start()
    precv[mm] = psend[mm]
    all_rows(LAST, sr.at[0]).wait_send()
    many(psend.at[0:n_mp - 1], precv.at[0:n_mp - 1], ps.at[0], pr.at[0]).wait_recv()
    for a in range(TYPES):
        typed = precv[0, a].astype(F32)
        for p in range(1, n_mp):
            typed = typed + precv[p, a].astype(F32)
        out[a] = jnp.maximum(typed, 0.0).astype(BF16)
    many(psend.at[0:n_mp - 1], precv.at[0:n_mp - 1], ps.at[0], pr.at[0]).wait_send()


def solution(mesh):
    n_mp = mesh.shape["mp"]

    def per_device(features, weights, sample_owner, sample_row, edge_src, edge_dst, edge_count):
        return pl.pallas_call(
            kernel,
            out_shape=pltpu.VMEM((TYPES, 64, SEEDS), BF16),
            in_specs=[pl.BlockSpec(memory_space=pltpu.HBM)] * 7,
            out_specs=pl.BlockSpec(memory_space=pltpu.VMEM),
            scratch_shapes=[
                pltpu.VMEM((TYPES, 64, 2048), BF16),
                pltpu.VMEM((11, 64, 512), BF16),
                pltpu.VMEM((TYPES, 1, 2048), I32),
                pltpu.VMEM((TYPES, 2048), I32),
                pltpu.VMEM((RELS, 2048), I32),
                pltpu.VMEM((RELS, 2048), I32),
                pltpu.SMEM((1, RELS), I32),
                pltpu.VMEM((TYPES * DP, CAP), I32),
                pltpu.VMEM((DP, TYPES, CAP), I32),
                pltpu.VMEM((DP, TYPES, CAP), I32),
                pltpu.VMEM((TYPES, DP, 64, CAP), BF16),
                pltpu.VMEM((TYPES, DP, 64, CAP), BF16),
                pltpu.VMEM((TYPES, 16, 256), F32),
                pltpu.VMEM((RELS, 2048), F32),
                pltpu.VMEM((RELS, 2048), F32),
                pltpu.VMEM((256, 2048), BF16),
                pltpu.VMEM((16, 256, 384), BF16),
                pltpu.VMEM((len(LAST_RELS), 16, SEEDS), F32),
                pltpu.VMEM((TYPES, 256, SEEDS), BF16),
                pltpu.VMEM((TYPES, 512, 256), BF16),
                pltpu.VMEM((64, 2048), BF16),
                pltpu.VMEM((n_mp, TYPES, 64, SEEDS), BF16),
                pltpu.VMEM((n_mp, TYPES, 64, SEEDS), BF16),
                pltpu.SemaphoreType.DMA((7,)),
                pltpu.SemaphoreType.DMA((1,)),
                pltpu.SemaphoreType.DMA((8,)),
                pltpu.SemaphoreType.DMA((TYPES,)),
                pltpu.SemaphoreType.DMA((LAST,)),
                pltpu.SemaphoreType.DMA((NZ,)),
                pltpu.SemaphoreType.DMA((1,)),
                pltpu.SemaphoreType.DMA((1,)),
            ],
            compiler_params=pltpu.CompilerParams(
                collective_id=0, has_side_effects=True, vmem_limit_bytes=60000000),
        )(features, weights, jnp.transpose(sample_owner, (0, 2, 1)), sample_row,
          edge_src, edge_dst, jnp.transpose(edge_count, (1, 0)))

    return jax.shard_map(
        per_device,
        mesh=mesh,
        in_specs=(
            P(None, "mp", "dp"),
            P(None, "mp", None),
            P(None, "dp", None),
            P(None, "dp"),
            P(None, "dp"),
            P(None, "dp"),
            P(None, "dp"),
        ),
        out_specs=P(None, "mp", "dp"),
        check_vma=False,
    )
```
